32 devices in a mesh: dp: 2 (over z, core), tp: 16 (over x, y).
Axes of the slice: x: 4, y: 4, z: 1, core: 2. Of those that a mesh axis runs over, the one named last changes fastest.
The devices are a block of a 4x4x8 slice.
Arguments:
- x: bfloat16 [4096, 3072], P('dp'), parts along dimension 0
- dy: bfloat16 [4096, 3072], P('dp'), parts along dimension 0
- gate: bfloat16 [4096, 8192], P('dp', 'tp'), parts along dimension 0
- up: bfloat16 [4096, 8192], P('dp', 'tp'), parts along dimension 0
- w_gate: bfloat16 [3072, 8192], P(None, 'tp')
- w_up: bfloat16 [3072, 8192], P(None, 'tp')
- w_down: bfloat16 [8192, 3072], P('tp')
Outputs:
- output 1: bfloat16 [4096, 3072], P('dp'), parts along dimension 0
- output 2: bfloat16 [6144, 8192], P('dp', 'tp'), parts along dimension 0
- output 3: bfloat16 [6144, 8192], P('dp', 'tp'), parts along dimension 0
- output 4: bfloat16 [16384, 3072], P(('dp', 'tp')), parts along dimension 0
There are 2 independent parts. The reference program is written for one: setup_inputs(seed, part) draws one part's arguments, and reference() takes and returns one part's arrays. A program takes and returns all parts, laid end to end along the dimension named above; an argument that names none is the same for every part.
All inputs are finite; a program needn't handle non-finite values.
Results may differ from the reference program's by a relative error of at most 0.012.
Values are sent between devices in bfloat16 or wider.
A program may use at most 768 MiB of HBM per device.

```python
import jax
import jax.numpy as jnp

ROWS = 2048
D = 3072
FF = 8192


def act(gate, up):
    return jax.nn.silu(gate) * up


def setup_inputs(seed: int = 0, part: int = 0) -> dict:
    kx, ky, ka, kb, kg, ku, kd = jax.random.split(jax.random.key(seed), 7)
    kx, ky, ka, kb = (jax.random.fold_in(k, part) for k in (kx, ky, ka, kb))
    drawn = {
        "x": jax.random.normal(kx, (ROWS, D), jnp.float32),
        "dy": jax.random.normal(ky, (ROWS, D), jnp.float32),
        "gate": jax.random.normal(ka, (ROWS, FF), jnp.float32),
        "up": jax.random.normal(kb, (ROWS, FF), jnp.float32),
        "w_gate": jax.random.normal(kg, (D, FF), jnp.float32) * D**-0.5,
        "w_up": jax.random.normal(ku, (D, FF), jnp.float32) * D**-0.5,
        "w_down": jax.random.normal(kd, (FF, D), jnp.float32) * FF**-0.5,
    }
    return {k: v.astype(jnp.bfloat16) for k, v in drawn.items()}


def reference(x, dy, gate, up, w_gate, w_up, w_down):
    hidden, back = jax.vjp(act, gate.astype(jnp.float32), up.astype(jnp.float32))
    d_hidden = jnp.dot(dy, w_down.T, preferred_element_type=jnp.float32)
    d_gate, d_up = (g.astype(jnp.bfloat16) for g in back(d_hidden))
    dx = jnp.dot(d_gate, w_gate.T, preferred_element_type=jnp.float32) + jnp.dot(d_up, w_up.T, preferred_element_type=jnp.float32)
    dw_gate = jnp.dot(x.T, d_gate, preferred_element_type=jnp.float32)
    dw_up = jnp.dot(x.T, d_up, preferred_element_type=jnp.float32)
    dw_down = jnp.dot(hidden.astype(jnp.bfloat16).T, dy, preferred_element_type=jnp.float32)
    return tuple(g.astype(jnp.bfloat16) for g in (dx, dw_gate, dw_up, dw_down))
```

```python
import jax
import jax.numpy as jnp
from jax import lax
from jax.experimental import pallas as pl
from jax.experimental.pallas import tpu as pltpu
from jax.sharding import PartitionSpec as P

MESH = pl.DeviceIdType.MESH
F32, BF16 = jnp.float32, jnp.bfloat16
BLOCK = 256
COLS = 256
SLOTS = 4
SIDE = 4
NT = (((1,), (1,)), ((), ()))
NN = (((1,), (0,)), ((), ()))


def dot(a, b, dims):
    return lax.dot_general(a, b, dims, preferred_element_type=F32)


def kernel(
    x, dy, gate, up, w_gate, w_up, w_down,
    dx, o_gate, o_up, o_down,
    acc, acc2, major_send, major_recv, minor_send, minor_recv,
    d_gate, d_up, hidden_t, dy_in, gate_in, up_in, x_cols, dy_cols,
    w_sem, in_sem, cols_sem, rs_send_sem, rs_recv_sem, ag_send_sem, ag_recv_sem,
):
    rows, depth = x.shape
    blocks = rows // BLOCK
    big, small = BLOCK // SIDE, BLOCK // SIDE // SIDE
    half, quarter = depth // 2, depth // 4
    pieces = depth // COLS

    me = lax.axis_index("tp")
    px, py = lax.div(me, SIDE), lax.rem(me, SIDE)

    def wrap(k):
        return lax.rem(k + SIDE, SIDE)

    x_ring = [wrap(px + 1) * SIDE + py, wrap(px - 1) * SIDE + py]
    y_ring = [px * SIDE + wrap(py + 1), px * SIDE + wrap(py - 1)]
    major = [(px, x_ring), (py, y_ring)]
    minor = [(py, y_ring), (px, x_ring)]

    weights = [
        pltpu.make_async_copy(w_down, o_down, w_sem.at[0]),
        pltpu.make_async_copy(w_gate, o_gate, w_sem.at[1]),
        pltpu.make_async_copy(w_up, o_up, w_sem.at[2]),
    ]

    def inputs(b):
        slot = lax.rem(b, 2)
        here = pl.ds(pl.multiple_of(b * BLOCK, BLOCK), BLOCK)
        return [
            pltpu.make_async_copy(src.at[here], dst.at[slot], in_sem.at[slot, k])
            for k, (src, dst) in enumerate([(dy, dy_in), (gate, gate_in), (up, up_in)])
        ]

    def columns(k):
        slot = lax.rem(k, 2)
        here = pl.ds(pl.multiple_of(k * COLS, COLS), COLS)
        return [
            pltpu.make_async_copy(src.at[:, here], dst.at[slot], cols_sem.at[slot, j])
            for j, (src, dst) in enumerate([(x, x_cols), (dy, dy_cols)])
        ]

    weights[0].start()
    for c in inputs(0):
        c.start()
    weights[1].start()
    weights[2].start()

    barrier = pltpu.get_barrier_semaphore()
    for n in x_ring + y_ring:
        pl.semaphore_signal(barrier, inc=1, device_id={"tp": n}, device_id_type=MESH)
    pl.semaphore_wait(barrier, 4)

    def remote(src, dst, send, recv, to):
        return pltpu.make_async_remote_copy(
            src_ref=src, dst_ref=dst, send_sem=send, recv_sem=recv, device_id={"tp": to}, device_id_type=MESH
        )

    def rs(b, h, m, phase):
        slot = lax.rem(b, SLOTS)
        sent, got = ((major_send, major_recv), (minor_send, minor_recv))[phase]
        ring = (major, minor)[phase][h][1]
        return remote(
            sent.at[slot, h, m], got.at[slot, h, m],
            rs_send_sem.at[slot, phase, h, m], rs_recv_sem.at[slot, phase, h, m], ring[m % 2],
        )

    def place(b, h, phase, chunk, side):
        start = b * BLOCK + (chunk * big if phase == 0 else major[h][0] * big + chunk * small)
        size = big if phase == 0 else small
        return dx.at[pl.ds(pl.multiple_of(start, size), size), pl.ds(h * half + side * quarter, quarter)]

    def ag(b, h, m, phase):
        slot = lax.rem(b, SLOTS)
        at, ring = (major, minor)[phase][h]
        chunk = [at, at, at, at, wrap(at - 1), wrap(at + 1)][m]
        ref = place(b, h, phase, chunk, (0, 1, 1, 0, 0, 1)[m])
        return remote(ref, ref, ag_send_sem.at[slot, phase, h, m], ag_recv_sem.at[slot, phase, h, m], ring[m % 2])

    def source(b, h, phase, chunk, side):
        slot = lax.rem(b, SLOTS - 1)
        ref, size = ((acc, big), (acc2, small))[phase]
        return ref[slot, pl.ds(pl.multiple_of(chunk * size, size), size), pl.ds(h * half + side * quarter, quarter)]

    def scatter_first(b, phase):
        slot = lax.rem(b, SLOTS)
        sent = (major_send, minor_send)[phase]
        for h in range(2):
            at = (major, minor)[phase][h][0]
            chunks = [wrap(at + 2), wrap(at + 2), wrap(at + 1), wrap(at - 1)]
            for m in range(4):
                sent[slot, h, m] = source(b, h, phase, chunks[m], (0, 1, 1, 0)[m]).astype(BF16)
        for m in range(4):
            for h in range(2):
                rs(b, h, m, phase).start()

    def scatter_second(b, phase):
        slot = lax.rem(b, SLOTS)
        sent, got = ((major_send, major_recv), (minor_send, minor_recv))[phase]
        for h in range(2):
            at = (major, minor)[phase][h][0]
            for m in range(2):
                rs(b, h, m, phase).wait_recv()
                chunk = wrap(at + 1) if m == 0 else wrap(at - 1)
                sent[slot, h, 4 + m] = (source(b, h, phase, chunk, m) + got[slot, h, m].astype(F32)).astype(BF16)
        for h in range(2):
            for m in range(2):
                rs(b, h, 4 + m, phase).start()

    def total(b, h, phase, side):
        slot = lax.rem(b, SLOTS)
        got = (major_recv, minor_recv)[phase]
        at = (major, minor)[phase][h][0]
        parts = ((3, 4), (2, 5))[side]
        return source(b, h, phase, at, side) + got[slot, h, parts[0]].astype(F32) + got[slot, h, parts[1]].astype(F32)

    def scatter_done(b, phase):
        for h in range(2):
            for m in range(2, 6):
                rs(b, h, m, phase).wait_recv()
            for side in range(2):
                value = total(b, h, phase, side)
                if phase == 0:
                    acc2[lax.rem(b, SLOTS - 1), :, pl.ds(h * half + side * quarter, quarter)] = value
                else:
                    place(b, h, 1, minor[h][0], side)[...] = value.astype(BF16)

    def sends_done(b, make, phase):
        for h in range(2):
            for m in range(6):
                make(b, h, m, phase).wait_send()

    def gather_first(b, phase):
        for m in range(4):
            for h in range(2):
                ag(b, h, m, phase).start()

    def gather_second(b, phase):
        for h in range(2):
            for m in range(2):
                ag(b, h, m, phase).wait_recv()
                ag(b, h, 4 + m, phase).start()

    def gather_done(b, phase):
        for h in range(2):
            for m in range(2, 6):
                ag(b, h, m, phase).wait_recv()

    def term(b):
        slot, out = lax.rem(b, 2), lax.rem(b, SLOTS - 1)
        here = pl.ds(pl.multiple_of(b * BLOCK, BLOCK), BLOCK)
        for c in inputs(b):
            c.wait()

        @pl.when(b == 0)
        def _():
            weights[0].wait()

        @pl.when(b + 1 < blocks)
        def _():
            for c in inputs(b + 1):
                c.start()

        d_hidden = dot(dy_in[slot], o_down[...], NT)
        g, u = gate_in[slot].astype(F32), up_in[slot].astype(F32)
        s = jax.nn.sigmoid(g)
        silu = g * s
        dg = (d_hidden * u * (s * (1.0 + g * (1.0 - s)))).astype(BF16)
        du = (d_hidden * silu).astype(BF16)
        d_gate[here, :] = dg
        d_up[here, :] = du
        hidden_t[:, here] = (silu * u).astype(BF16).T

        @pl.when(b == 0)
        def _():
            weights[1].wait()
            weights[2].wait()

        for j in range(4):
            cut = pl.ds(j * quarter, quarter)
            acc[out, :, cut] = dot(d_gate[here, :], o_gate[cut, :], NT) + dot(d_up[here, :], o_up[cut, :], NT)

    def weight_gradients(k):
        slot = lax.rem(k, 2)
        here = pl.ds(pl.multiple_of(k * COLS, COLS), COLS)
        for c in columns(k):
            c.wait()

        @pl.when(k + 1 < pieces)
        def _():
            for c in columns(k + 1):
                c.start()

        x_t = x_cols[slot].T
        o_gate[here, :] = dot(x_t, d_gate[...], NN).astype(BF16)
        o_up[here, :] = dot(x_t, d_up[...], NN).astype(BF16)
        o_down[:, here] = dot(hidden_t[...], dy_cols[slot], NN).astype(BF16)

    per_step = 2
    first_step = blocks

    def at(i, lag, f):
        b = i - lag

        @pl.when(jnp.logical_and(b >= 0, b < blocks))
        def _():
            f(b)

    def weights_at(i, j):
        k = (i - first_step) * per_step + j

        @pl.when(jnp.logical_and(i >= first_step, k < pieces))
        def _():
            weight_gradients(k)

    def step(i, carry):
        at(i, 4, lambda b: sends_done(b, rs, 0))

        @pl.when(i < blocks)
        def _():
            term(i)
            scatter_first(i, 0)

        @pl.when(i == first_step - 1)
        def _():
            for c in columns(0):
                c.start()

        def last(b):
            gather_done(b, 0)
            sends_done(b, ag, 0)

        at(i, 8, last)
        at(i, 7, lambda b: gather_second(b, 0))

        def gather_rows(b):
            gather_done(b, 1)
            sends_done(b, ag, 1)
            gather_first(b, 0)

        at(i, 6, gather_rows)
        weights_at(i, 0)
        at(i, 5, lambda b: gather_second(b, 1))

        def finish(b):
            scatter_done(b, 1)
            gather_first(b, 1)

        at(i, 4, finish)
        at(i, 3, lambda b: scatter_second(b, 1))
        at(i, 6, lambda b: sends_done(b, rs, 1))
        weights_at(i, 1)

        def turn(b):
            scatter_done(b, 0)
            scatter_first(b, 1)

        at(i, 2, turn)
        at(i, 1, lambda b: scatter_second(b, 0))
        return carry

    lax.fori_loop(0, blocks + 8, step, 0)


def write_out(dx, a, b, c, o_dx, o_a, o_b, o_c, sem):
    copies = []
    for src, dst in ((dx, o_dx), (a, o_a), (b, o_b), (c, o_c)):
        n = src.shape[0] // 4
        for j in range(4):
            cut = pl.ds(j * n, n)
            copies.append(pltpu.make_async_copy(src.at[cut], dst.at[cut], sem.at[len(copies)]))
    for c in copies:
        c.start()
    for c in copies:
        c.wait()


def solution(mesh):
    assert mesh.shape["tp"] == SIDE * SIDE

    def step(x, dy, gate, up, w_gate, w_up, w_down):
        rows, depth = x.shape
        units = gate.shape[1]
        big, small, quarter = BLOCK // SIDE, BLOCK // SIDE // SIDE, depth // 4
        outs = [x, w_gate, w_up, w_down]
        dma = pltpu.SemaphoreType.DMA
        flops = 2 * 6 * rows * depth * units
        result = pl.pallas_call(
            kernel,
            out_shape=[pltpu.VMEM(o.shape, BF16) for o in outs],
            in_specs=[pl.BlockSpec(memory_space=pltpu.HBM)] * 7,
            out_specs=[pl.BlockSpec(memory_space=pltpu.VMEM)] * 4,
            scratch_shapes=[
                pltpu.VMEM((SLOTS - 1, BLOCK, depth), F32),
                pltpu.VMEM((SLOTS - 1, big, depth), F32),
                pltpu.VMEM((SLOTS, 2, 6, big, quarter), BF16),
                pltpu.VMEM((SLOTS, 2, 6, big, quarter), BF16),
                pltpu.VMEM((SLOTS, 2, 6, small, quarter), BF16),
                pltpu.VMEM((SLOTS, 2, 6, small, quarter), BF16),
                pltpu.VMEM((rows, units), BF16),
                pltpu.VMEM((rows, units), BF16),
                pltpu.VMEM((units, rows), BF16),
                pltpu.VMEM((2, BLOCK, depth), BF16),
                pltpu.VMEM((2, BLOCK, units), BF16),
                pltpu.VMEM((2, BLOCK, units), BF16),
                pltpu.VMEM((2, rows, COLS), BF16),
                pltpu.VMEM((2, rows, COLS), BF16),
                dma((3,)),
                dma((2, 3)),
                dma((2, 2)),
                dma((SLOTS, 2, 2, 6)),
                dma((SLOTS, 2, 2, 6)),
                dma((SLOTS, 2, 2, 6)),
                dma((SLOTS, 2, 2, 6)),
            ],
            compiler_params=pltpu.CompilerParams(
                collective_id=0, has_side_effects=True, vmem_limit_bytes=42 * 2**20
            ),
            cost_estimate=pl.CostEstimate(flops=flops, bytes_accessed=60 * 2**20, transcendentals=rows * units),
        )(x, dy, gate, up, w_gate, w_up, w_down)
        return pl.pallas_call(
            write_out,
            out_shape=[pltpu.HBM(o.shape, BF16) for o in outs],
            in_specs=[pl.BlockSpec(memory_space=pltpu.VMEM)] * 4,
            out_specs=[pl.BlockSpec(memory_space=pltpu.HBM)] * 4,
            scratch_shapes=[dma((16,))],
            compiler_params=pltpu.CompilerParams(has_side_effects=True, vmem_limit_bytes=2**20),
        )(*result)

    tokens, columns, rows = P("dp", None), P(None, "tp"), P("tp", None)
    return jax.shard_map(
        step,
        mesh=mesh,
        in_specs=(tokens, tokens, P("dp", "tp"), P("dp", "tp"), columns, columns, rows),
        out_specs=(tokens, P("dp", "tp"), P("dp", "tp"), P(("dp", "tp"), None)),
        check_vma=False,
    )
```

```python
import jax
import jax.numpy as jnp
from jax import lax
from jax.experimental import pallas as pl
from jax.experimental.pallas import tpu as pltpu
from jax.sharding import PartitionSpec as P

MESH = pl.DeviceIdType.MESH
F32, BF16 = jnp.float32, jnp.bfloat16
BLOCK = 256
COLS = 256
SLOTS = 4
SIDE = 4
ORDER = (0, 2, 1, 3)
NT = (((1,), (1,)), ((), ()))
NN = (((1,), (0,)), ((), ()))


def dot(a, b, dims):
    return lax.dot_general(a, b, dims, preferred_element_type=F32)


def kernel(
    x, dy, gate, up, w_gate, w_up, w_down,
    dx, o_gate, o_up, o_down,
    acc, acc2, major_send, major_recv, minor_send, minor_recv,
    d_gate, d_up, hidden_t, dy_in, gate_in, up_in, x_cols, dy_cols,
    w_sem, in_sem, cols_sem, rs_send_sem, rs_recv_sem, ag_send_sem, ag_recv_sem,
):
    rows, depth = x.shape
    blocks = rows // BLOCK
    big, small = BLOCK // SIDE, BLOCK // SIDE // SIDE
    half, quarter = depth // 2, depth // 4
    pieces = depth // COLS

    me = lax.axis_index("tp")
    px, py = lax.div(me, SIDE), lax.rem(me, SIDE)

    def wrap(k):
        return lax.rem(k + SIDE, SIDE)

    x_ring = [wrap(px + 1) * SIDE + py, wrap(px - 1) * SIDE + py]
    y_ring = [px * SIDE + wrap(py + 1), px * SIDE + wrap(py - 1)]
    major = [(px, x_ring), (py, y_ring)]
    minor = [(py, y_ring), (px, x_ring)]

    quarters = [pl.ds(j * quarter, quarter) for j in range(4)]
    down_in = [pltpu.make_async_copy(w_down.at[:, c], o_down.at[:, c], w_sem.at[0, j]) for j, c in enumerate(quarters)]
    gate_up_in = [
        [pltpu.make_async_copy(src.at[c], dst.at[c], w_sem.at[k, j]) for k, (src, dst) in enumerate([(w_gate, o_gate), (w_up, o_up)], 1)]
        for j, c in enumerate(quarters)
    ]

    def inputs(b):
        slot = lax.rem(b, 2)
        here = pl.ds(pl.multiple_of(b * BLOCK, BLOCK), BLOCK)
        return [
            pltpu.make_async_copy(src.at[here], dst.at[slot], in_sem.at[slot, k])
            for k, (src, dst) in enumerate([(gate, gate_in), (up, up_in)])
        ]

    def dy_block(b):
        slot = lax.rem(b, 2)
        here = pl.ds(pl.multiple_of(b * BLOCK, BLOCK), BLOCK)
        return [
            pltpu.make_async_copy(dy.at[here, c], dy_in.at[slot, :, c], in_sem.at[slot, 2 + j])
            for j, c in enumerate(quarters)
        ]

    def columns(k):
        slot = lax.rem(k, 2)
        here = pl.ds(pl.multiple_of(k * COLS, COLS), COLS)
        return [
            pltpu.make_async_copy(src.at[:, here], dst.at[slot], cols_sem.at[slot, j])
            for j, (src, dst) in enumerate([(x, x_cols), (dy, dy_cols)])
        ]

    for c in inputs(0):
        c.start()
    for pair in zip(down_in, dy_block(0)):
        for c in pair:
            c.start()
    for j in ORDER:
        for c in gate_up_in[j]:
            c.start()

    barrier = pltpu.get_barrier_semaphore()
    for n in x_ring + y_ring:
        pl.semaphore_signal(barrier, inc=1, device_id={"tp": n}, device_id_type=MESH)

    def remote(src, dst, send, recv, to):
        return pltpu.make_async_remote_copy(
            src_ref=src, dst_ref=dst, send_sem=send, recv_sem=recv, device_id={"tp": to}, device_id_type=MESH
        )

    def rs(b, h, m, phase):
        slot = lax.rem(b, SLOTS)
        sent, got = ((major_send, major_recv), (minor_send, minor_recv))[phase]
        ring = (major, minor)[phase][h][1]
        return remote(
            sent.at[slot, h, m], got.at[slot, h, m],
            rs_send_sem.at[slot, phase], rs_recv_sem.at[slot, phase, int(m >= 2)], ring[m % 2],
        )

    def taken(ref, sem):
        pltpu.make_async_copy(ref, ref, sem).wait()

    def rs_got(b, phase, late):
        slot = lax.rem(b, SLOTS)
        got = (major_recv, minor_recv)[phase]
        taken(got.at[slot, :, pl.ds(2, 4) if late else pl.ds(0, 2)], rs_recv_sem.at[slot, phase, late])

    def rs_left(b, phase):
        slot = lax.rem(b, SLOTS)
        taken((major_send, minor_send)[phase].at[slot], rs_send_sem.at[slot, phase])

    def ag_left(b, phase):
        slot = lax.rem(b, SLOTS)
        taken((major_send, minor_send)[phase].at[slot], ag_send_sem.at[slot, phase])

    def ag_got(b, phase):
        slot = lax.rem(b, SLOTS)
        taken((major_recv, minor_recv)[phase].at[slot, :, pl.ds(2, 4)], ag_recv_sem.at[slot, phase, 4])

    def place(b, h, phase, chunk, side):
        start = b * BLOCK + (chunk * big if phase == 0 else major[h][0] * big + chunk * small)
        size = big if phase == 0 else small
        return dx.at[pl.ds(pl.multiple_of(start, size), size), pl.ds(h * half + side * quarter, quarter)]

    def ag(b, h, m, phase):
        slot = lax.rem(b, SLOTS)
        at, ring = (major, minor)[phase][h]
        chunk = [at, at, at, at, wrap(at - 1), wrap(at + 1)][m]
        ref = place(b, h, phase, chunk, (0, 1, 1, 0, 0, 1)[m])
        return remote(ref, ref, ag_send_sem.at[slot, phase], ag_recv_sem.at[slot, phase, 2 * h + m if m < 2 else 4], ring[m % 2])

    def source(b, h, phase, chunk, side):
        slot = lax.rem(b, SLOTS - 1)
        ref, size = ((acc, big), (acc2, small))[phase]
        return ref[slot, pl.ds(pl.multiple_of(chunk * size, size), size), pl.ds(h * half + side * quarter, quarter)]

    def scatter_first(b, phase, hs=(0, 1), ms=(0, 1, 2, 3)):
        slot = lax.rem(b, SLOTS)
        sent = (major_send, minor_send)[phase]
        for h in hs:
            at = (major, minor)[phase][h][0]
            chunks = [wrap(at + 2), wrap(at + 2), wrap(at + 1), wrap(at - 1)]
            for m in ms:
                sent[slot, h, m] = source(b, h, phase, chunks[m], (0, 1, 1, 0)[m]).astype(BF16)
        for m in ms:
            for h in hs:
                rs(b, h, m, phase).start()

    def scatter_second(b, phase):
        slot = lax.rem(b, SLOTS)
        sent, got = ((major_send, major_recv), (minor_send, minor_recv))[phase]
        rs_got(b, phase, 0)
        for h in range(2):
            at = (major, minor)[phase][h][0]
            for m in range(2):
                chunk = wrap(at + 1) if m == 0 else wrap(at - 1)
                sent[slot, h, 4 + m] = (source(b, h, phase, chunk, m) + got[slot, h, m].astype(F32)).astype(BF16)
        for h in range(2):
            for m in range(2):
                rs(b, h, 4 + m, phase).start()

    def total(b, h, phase, side):
        slot = lax.rem(b, SLOTS)
        got = (major_recv, minor_recv)[phase]
        at = (major, minor)[phase][h][0]
        parts = ((3, 4), (2, 5))[side]
        return source(b, h, phase, at, side) + got[slot, h, parts[0]].astype(F32) + got[slot, h, parts[1]].astype(F32)

    def scatter_done(b, phase):
        rs_got(b, phase, 1)
        for h in range(2):
            for side in range(2):
                value = total(b, h, phase, side)
                if phase == 0:
                    acc2[lax.rem(b, SLOTS - 1), :, pl.ds(h * half + side * quarter, quarter)] = value
                else:
                    place(b, h, 1, minor[h][0], side)[...] = value.astype(BF16)

    def gather_first(b, phase):
        for m in range(4):
            for h in range(2):
                ag(b, h, m, phase).start()

    def gather_second(b, phase):
        for h in range(2):
            for m in range(2):
                ag(b, h, m, phase).wait_recv()
                ag(b, h, 4 + m, phase).start()

    def term(b):
        slot, out = lax.rem(b, 2), lax.rem(b, SLOTS - 1)
        here = pl.ds(pl.multiple_of(b * BLOCK, BLOCK), BLOCK)
        for c in inputs(b):
            c.wait()
        g, u = gate_in[slot].astype(F32), up_in[slot].astype(F32)
        s = jax.nn.sigmoid(g)
        silu = g * s
        slope = s * (1.0 + g * (1.0 - s))
        hidden_t[:, here] = (silu * u).astype(BF16).T
        d_hidden = None
        for j, c in enumerate(dy_block(b)):
            c.wait()

            @pl.when(b == 0)
            def _(j=j):
                down_in[j].wait()

            part = dot(dy_in[slot, :, quarters[j]], o_down[:, quarters[j]], NT)
            d_hidden = part if d_hidden is None else d_hidden + part
        d_gate[here, :] = (d_hidden * u * slope).astype(BF16)
        d_up[here, :] = (d_hidden * silu).astype(BF16)

        @pl.when(b + 1 < blocks)
        def _():
            for c in dy_block(b + 1) + inputs(b + 1):
                c.start()

        @pl.when(b == 0)
        def _():
            pl.semaphore_wait(barrier, 4)

        for j in ORDER:

            @pl.when(b == 0)
            def _(j=j):
                for c in gate_up_in[j]:
                    c.wait()

            cut = quarters[j]
            acc[out, :, cut] = dot(d_gate[here, :], o_gate[cut, :], NT) + dot(d_up[here, :], o_up[cut, :], NT)
            scatter_first(b, 0, (j // 2,), ((0, 3), (1, 2))[j % 2])

    def weight_gradients(k):
        slot = lax.rem(k, 2)
        here = pl.ds(pl.multiple_of(k * COLS, COLS), COLS)
        for c in columns(k):
            c.wait()

        @pl.when(k + 1 < pieces)
        def _():
            for c in columns(k + 1):
                c.start()

        x_t = x_cols[slot].T
        o_gate[here, :] = dot(x_t, d_gate[...], NN).astype(BF16)
        o_up[here, :] = dot(x_t, d_up[...], NN).astype(BF16)
        o_down[:, here] = dot(hidden_t[...], dy_cols[slot], NN).astype(BF16)

    per_step = 2
    first_step = blocks

    def at(i, lag, f):
        b = i - lag

        @pl.when(jnp.logical_and(b >= 0, b < blocks))
        def _():
            f(b)

    def weights_at(i, j):
        k = (i - first_step) * per_step + j

        @pl.when(jnp.logical_and(i >= first_step, k < pieces))
        def _():
            weight_gradients(k)

    def step(i, carry):
        at(i, 4, lambda b: rs_left(b, 0))

        @pl.when(i < blocks)
        def _():
            term(i)

        @pl.when(i == first_step - 1)
        def _():
            for c in columns(0):
                c.start()

        def turn(b):
            scatter_done(b, 0)
            scatter_first(b, 1)

        at(i, 6, lambda b: rs_left(b, 1))
        at(i, 2, turn)
        at(i, 1, lambda b: scatter_second(b, 0))

        def finish(b):
            scatter_done(b, 1)
            gather_first(b, 1)

        at(i, 8, lambda b: ag_left(b, 1))
        at(i, 4, finish)
        at(i, 3, lambda b: scatter_second(b, 1))
        weights_at(i, 0)
        at(i, 5, lambda b: gather_second(b, 1))
        at(i, 7, lambda b: gather_second(b, 0))

        def gather_rows(b):
            ag_got(b, 1)
            gather_first(b, 0)

        at(i, 6, gather_rows)
        weights_at(i, 1)

        def last(b):
            ag_got(b, 0)
            ag_left(b, 0)

        at(i, 8, last)
        return carry

    lax.fori_loop(0, blocks + 8, step, 0)


def write_out(dx, a, b, c, o_dx, o_a, o_b, o_c, sem):
    copies = []
    for src, dst in ((dx, o_dx), (a, o_a), (b, o_b), (c, o_c)):
        n = src.shape[0] // 4
        for j in range(4):
            cut = pl.ds(j * n, n)
            copies.append(pltpu.make_async_copy(src.at[cut], dst.at[cut], sem.at[len(copies)]))
    for c in copies:
        c.start()
    for c in copies:
        c.wait()


def solution(mesh):
    assert mesh.shape["tp"] == SIDE * SIDE

    def step(x, dy, gate, up, w_gate, w_up, w_down):
        rows, depth = x.shape
        units = gate.shape[1]
        big, small, quarter = BLOCK // SIDE, BLOCK // SIDE // SIDE, depth // 4
        outs = [x, w_gate, w_up, w_down]
        dma = pltpu.SemaphoreType.DMA
        flops = 2 * 6 * rows * depth * units
        result = pl.pallas_call(
            kernel,
            out_shape=[pltpu.VMEM(o.shape, BF16) for o in outs],
            in_specs=[pl.BlockSpec(memory_space=pltpu.HBM)] * 7,
            out_specs=[pl.BlockSpec(memory_space=pltpu.VMEM)] * 4,
            scratch_shapes=[
                pltpu.VMEM((SLOTS - 1, BLOCK, depth), F32),
                pltpu.VMEM((SLOTS - 1, big, depth), F32),
                pltpu.VMEM((SLOTS, 2, 6, big, quarter), BF16),
                pltpu.VMEM((SLOTS, 2, 6, big, quarter), BF16),
                pltpu.VMEM((SLOTS, 2, 6, small, quarter), BF16),
                pltpu.VMEM((SLOTS, 2, 6, small, quarter), BF16),
                pltpu.VMEM((rows, units), BF16),
                pltpu.VMEM((rows, units), BF16),
                pltpu.VMEM((units, rows), BF16),
                pltpu.VMEM((2, BLOCK, depth), BF16),
                pltpu.VMEM((2, BLOCK, units), BF16),
                pltpu.VMEM((2, BLOCK, units), BF16),
                pltpu.VMEM((2, rows, COLS), BF16),
                pltpu.VMEM((2, rows, COLS), BF16),
                dma((3, 4)),
                dma((2, 6)),
                dma((2, 2)),
                dma((SLOTS, 2)),
                dma((SLOTS, 2, 2)),
                dma((SLOTS, 2)),
                dma((SLOTS, 2, 5)),
            ],
            compiler_params=pltpu.CompilerParams(
                collective_id=0, has_side_effects=True, vmem_limit_bytes=42 * 2**20
            ),
            cost_estimate=pl.CostEstimate(flops=flops, bytes_accessed=60 * 2**20, transcendentals=rows * units),
        )(x, dy, gate, up, w_gate, w_up, w_down)
        return pl.pallas_call(
            write_out,
            out_shape=[pltpu.HBM(o.shape, BF16) for o in outs],
            in_specs=[pl.BlockSpec(memory_space=pltpu.VMEM)] * 4,
            out_specs=[pl.BlockSpec(memory_space=pltpu.HBM)] * 4,
            scratch_shapes=[dma((16,))],
            compiler_params=pltpu.CompilerParams(has_side_effects=True, vmem_limit_bytes=2**20),
        )(*result)

    tokens, columns, rows = P("dp", None), P(None, "tp"), P("tp", None)
    return jax.shard_map(
        step,
        mesh=mesh,
        in_specs=(tokens, tokens, P("dp", "tp"), P("dp", "tp"), columns, columns, rows),
        out_specs=(tokens, P("dp", "tp"), P("dp", "tp"), P(("dp", "tp"), None)),
        check_vma=False,
    )
```

```python
import jax
import jax.numpy as jnp
from jax import lax
from jax.experimental import pallas as pl
from jax.experimental.pallas import tpu as pltpu
from jax.sharding import PartitionSpec as P

MESH = pl.DeviceIdType.MESH
F32, BF16 = jnp.float32, jnp.bfloat16
BLOCK = 256
COLS = 256
SLOTS = 4
SIDE = 4
ORDER = (0, 2, 1, 3)
NT = (((1,), (1,)), ((), ()))
NN = (((1,), (0,)), ((), ()))


def dot(a, b, dims):
    return lax.dot_general(a, b, dims, preferred_element_type=F32)


def kernel(
    x, dy, gate, up, w_gate, w_up, w_down,
    dx, o_gate, o_up, o_down,
    acc, acc2, major_send, major_recv, minor_send, minor_recv,
    d_gate, d_up, hidden_t, dy_in, gate_in, up_in, x_cols, dy_cols,
    first_sem, w_sem, in_sem, cols_sem, rs_send_sem, rs_recv_sem, ag_send_sem, ag_major_sem, ag_minor_sem,
):
    rows, depth = x.shape
    blocks = rows // BLOCK
    big, small = BLOCK // SIDE, BLOCK // SIDE // SIDE
    half, quarter = depth // 2, depth // 4
    pieces = depth // COLS
    units = gate.shape[1]

    me = lax.axis_index("tp")
    px, py = lax.div(me, SIDE), lax.rem(me, SIDE)

    def wrap(k):
        return lax.rem(k + SIDE, SIDE)

    x_ring = [wrap(px + 1) * SIDE + py, wrap(px - 1) * SIDE + py]
    y_ring = [px * SIDE + wrap(py + 1), px * SIDE + wrap(py - 1)]
    major = [(px, x_ring), (py, y_ring)]
    minor = [(py, y_ring), (px, x_ring)]

    def taken(ref, sem):
        pltpu.make_async_copy(ref, ref, sem).wait()

    def taken_rows(n, sem):
        taken(d_gate.at[pl.ds(0, n)], sem)

    quarters = [pl.ds(j * quarter, quarter) for j in range(4)]

    def weight_quarter(j):
        c = quarters[j]
        for src, dst in ((w_gate, o_gate), (w_up, o_up)):
            pltpu.make_async_copy(src.at[c], dst.at[c], w_sem.at[j]).start()

    def inputs(b):
        slot = lax.rem(b, 2)
        here = pl.ds(pl.multiple_of(b * BLOCK, BLOCK), BLOCK)
        for src, dst in ((dy, dy_in), (gate, gate_in), (up, up_in)):
            pltpu.make_async_copy(src.at[here], dst.at[slot], in_sem.at[slot]).start()

    def columns(k):
        slot = lax.rem(k, 2)
        here = pl.ds(pl.multiple_of(k * COLS, COLS), COLS)
        for src, dst in ((x, x_cols), (dy, dy_cols)):
            pltpu.make_async_copy(src.at[:, here], dst.at[slot], cols_sem.at[slot]).start()

    for src, dst in ((gate, gate_in), (up, up_in)):
        pltpu.make_async_copy(src.at[pl.ds(0, BLOCK)], dst.at[0], first_sem.at[4]).start()
    for j, c in enumerate(quarters):
        pltpu.make_async_copy(w_down.at[:, c], o_down.at[:, c], first_sem.at[j]).start()
        pltpu.make_async_copy(dy.at[pl.ds(0, BLOCK), c], dy_in.at[0, :, c], first_sem.at[j]).start()

    barrier = pltpu.get_barrier_semaphore()
    for n in x_ring + y_ring:
        pl.semaphore_signal(barrier, inc=1, device_id={"tp": n}, device_id_type=MESH)

    def remote(src, dst, send, recv, to):
        return pltpu.make_async_remote_copy(
            src_ref=src, dst_ref=dst, send_sem=send, recv_sem=recv, device_id={"tp": to}, device_id_type=MESH
        )

    def rs(b, h, m, phase):
        slot = lax.rem(b, SLOTS)
        sent, got = ((major_send, major_recv), (minor_send, minor_recv))[phase]
        ring = (major, minor)[phase][h][1]
        return remote(
            sent.at[slot, h, m], got.at[slot, h, m],
            rs_send_sem.at[slot, phase], rs_recv_sem.at[slot, phase, int(m >= 2)], ring[m % 2],
        )

    def rs_got(b, phase, late):
        slot = lax.rem(b, SLOTS)
        got = (major_recv, minor_recv)[phase]
        taken(got.at[slot, :, pl.ds(2, 4) if late else pl.ds(0, 2)], rs_recv_sem.at[slot, phase, late])

    def rs_left(b, phase):
        slot = lax.rem(b, SLOTS)
        taken((major_send, minor_send)[phase].at[slot], rs_send_sem.at[slot, phase])

    def ag_left(b, phase):
        slot = lax.rem(b, SLOTS)
        taken((major_send, minor_send)[phase].at[slot], ag_send_sem.at[slot, phase])

    def ag_sem(b, h, m, phase):
        if phase == 0:
            return ag_major_sem.at[lax.rem(b, SLOTS + 1), h if m < 2 else 2]
        return ag_minor_sem.at[lax.rem(b, SLOTS), int(m >= 2)]

    def ag_got(b, phase):
        taken((major_recv, minor_recv)[phase].at[lax.rem(b, SLOTS), :, pl.ds(2, 4)], ag_sem(b, 0, 2, phase))

    def place(b, h, phase, chunk, side):
        start = b * BLOCK + (chunk * big if phase == 0 else major[h][0] * big + chunk * small)
        size = big if phase == 0 else small
        return dx.at[pl.ds(pl.multiple_of(start, size), size), pl.ds(h * half + side * quarter, quarter)]

    def ag(b, h, m, phase):
        slot = lax.rem(b, SLOTS)
        at, ring = (major, minor)[phase][h]
        chunk = [at, at, at, at, wrap(at - 1), wrap(at + 1)][m]
        ref = place(b, h, phase, chunk, (0, 1, 1, 0, 0, 1)[m])
        return remote(ref, ref, ag_send_sem.at[slot, phase], ag_sem(b, h, m, phase), ring[m % 2])

    def source(b, h, phase, chunk, side):
        slot = lax.rem(b, SLOTS - 1)
        ref, size = ((acc, big), (acc2, small))[phase]
        return ref[slot, pl.ds(pl.multiple_of(chunk * size, size), size), pl.ds(h * half + side * quarter, quarter)]

    def scatter_first(b, phase, hs=(0, 1), ms=(0, 1, 2, 3)):
        slot = lax.rem(b, SLOTS)
        sent = (major_send, minor_send)[phase]
        for h in hs:
            at = (major, minor)[phase][h][0]
            chunks = [wrap(at + 2), wrap(at + 2), wrap(at + 1), wrap(at - 1)]
            for m in ms:
                sent[slot, h, m] = source(b, h, phase, chunks[m], (0, 1, 1, 0)[m]).astype(BF16)
        for m in ms:
            for h in hs:
                rs(b, h, m, phase).start()

    def scatter_second(b, phase):
        slot = lax.rem(b, SLOTS)
        sent, got = ((major_send, major_recv), (minor_send, minor_recv))[phase]
        rs_got(b, phase, 0)
        for h in range(2):
            at = (major, minor)[phase][h][0]
            for m in range(2):
                chunk = wrap(at + 1) if m == 0 else wrap(at - 1)
                sent[slot, h, 4 + m] = (source(b, h, phase, chunk, m) + got[slot, h, m].astype(F32)).astype(BF16)
        for h in range(2):
            for m in range(2):
                rs(b, h, 4 + m, phase).start()

    def total(b, h, phase, side):
        slot = lax.rem(b, SLOTS)
        got = (major_recv, minor_recv)[phase]
        at = (major, minor)[phase][h][0]
        parts = ((3, 4), (2, 5))[side]
        return source(b, h, phase, at, side) + got[slot, h, parts[0]].astype(F32) + got[slot, h, parts[1]].astype(F32)

    def scatter_done(b, phase):
        rs_got(b, phase, 1)
        for h in range(2):
            for side in range(2):
                value = total(b, h, phase, side)
                if phase == 0:
                    acc2[lax.rem(b, SLOTS - 1), :, pl.ds(h * half + side * quarter, quarter)] = value
                else:
                    place(b, h, 1, minor[h][0], side)[...] = value.astype(BF16)

    def gather_first(b, phase):
        for m in range(4):
            for h in range(2):
                ag(b, h, m, phase).start()

    def gather_second(b, phase):
        if phase == 1:
            taken(minor_recv.at[lax.rem(b, SLOTS), :, pl.ds(0, 2)], ag_sem(b, 0, 0, 1))
        for h in range(2):
            if phase == 0:
                taken(major_recv.at[lax.rem(b, SLOTS), 0, pl.ds(0, 2)], ag_sem(b, h, 0, 0))
            for m in range(2):
                ag(b, h, 4 + m, phase).start()

    def activation(slot, rows):
        g, u = gate_in[slot, rows].astype(F32), up_in[slot, rows].astype(F32)
        s = jax.nn.sigmoid(g)
        silu = g * s
        return u, silu, s * (1.0 + g * (1.0 - s)), (silu * u).astype(BF16)

    def term(b):
        slot, out = lax.rem(b, 2), lax.rem(b, SLOTS - 1)
        here = pl.ds(pl.multiple_of(b * BLOCK, BLOCK), BLOCK)

        @pl.when(b == 0)
        def _():
            taken_rows(2 * BLOCK, first_sem.at[4])

        @pl.when(b > 0)
        def _():
            taken_rows(BLOCK * (depth + 2 * units) // units, in_sem.at[slot])

        u, silu, slope, hidden = activation(slot, pl.ds(0, BLOCK))
        hidden_t[:, here] = hidden.T
        d_hidden = None
        for j, c in enumerate(quarters):

            @pl.when(b == 0)
            def _(j=j):
                taken_rows((units + BLOCK) * quarter // units, first_sem.at[j])
                if j == 0:
                    for k in ORDER:
                        weight_quarter(k)

            piece = dot(dy_in[slot, :, c], o_down[:, c], NT)
            d_hidden = piece if d_hidden is None else d_hidden + piece
        d_gate[here, :] = (d_hidden * u * slope).astype(BF16)
        d_up[here, :] = (d_hidden * silu).astype(BF16)
        pl.when(b + 1 < blocks)(lambda: inputs(b + 1))

        @pl.when(b == 0)
        def _():
            pl.semaphore_wait(barrier, 4)

        for j in ORDER:

            @pl.when(b == 0)
            def _(j=j):
                taken_rows(2 * quarter, w_sem.at[j])

            cut = quarters[j]
            acc[out, :, cut] = dot(d_gate[here, :], o_gate[cut, :], NT) + dot(d_up[here, :], o_up[cut, :], NT)
            scatter_first(b, 0, (j // 2,), ((0, 3), (1, 2))[j % 2])

    def weight_gradients(k):
        slot = lax.rem(k, 2)
        here = pl.ds(pl.multiple_of(k * COLS, COLS), COLS)
        taken_rows(2 * rows * COLS // units, cols_sem.at[slot])
        pl.when(k + 1 < pieces)(lambda: columns(k + 1))

        x_t = x_cols[slot].T
        o_gate[here, :] = dot(x_t, d_gate[...], NN).astype(BF16)
        o_up[here, :] = dot(x_t, d_up[...], NN).astype(BF16)
        o_down[:, here] = dot(hidden_t[...], dy_cols[slot], NN).astype(BF16)

    per_step = 2
    first_step = blocks

    def at(i, lag, f):
        b = i - lag

        @pl.when(jnp.logical_and(b >= 0, b < blocks))
        def _():
            f(b)

    def weights_at(i, j):
        k = (i - first_step) * per_step + j

        @pl.when(jnp.logical_and(i >= first_step, k < pieces))
        def _():
            weight_gradients(k)

    def step(i, carry):
        at(i, 4, lambda b: rs_left(b, 0))

        pl.when(i < blocks)(lambda: term(i))
        pl.when(i == first_step - 1)(lambda: columns(0))

        def turn(b):
            scatter_done(b, 0)
            scatter_first(b, 1)

        at(i, 6, lambda b: rs_left(b, 1))
        at(i, 2, turn)
        at(i, 1, lambda b: scatter_second(b, 0))

        def finish(b):
            scatter_done(b, 1)
            gather_first(b, 1)

        at(i, 8, lambda b: ag_left(b, 1))
        at(i, 4, finish)
        at(i, 3, lambda b: scatter_second(b, 1))
        weights_at(i, 0)
        at(i, 5, lambda b: gather_second(b, 1))
        def gather_rows(b):
            ag_got(b, 1)
            gather_first(b, 0)

        at(i, 6, gather_rows)
        at(i, 7, lambda b: gather_second(b, 0))

        weights_at(i, 1)

        def last(b):
            ag_got(b, 0)
            ag_left(b, 0)

        at(i, 8, last)
        return carry

    lax.fori_loop(0, blocks + 8, step, 0)


def write_out(dx, a, b, c, o_dx, o_a, o_b, o_c, sem):
    copies = []
    for src, dst in ((dx, o_dx), (a, o_a), (b, o_b), (c, o_c)):
        n = src.shape[0] // 4
        for j in range(4):
            cut = pl.ds(j * n, n)
            copies.append(pltpu.make_async_copy(src.at[cut], dst.at[cut], sem.at[len(copies)]))
    for c in copies:
        c.start()
    for c in copies:
        c.wait()


def solution(mesh):
    assert mesh.shape["tp"] == SIDE * SIDE

    def step(x, dy, gate, up, w_gate, w_up, w_down):
        rows, depth = x.shape
        units = gate.shape[1]
        big, small, quarter = BLOCK // SIDE, BLOCK // SIDE // SIDE, depth // 4
        outs = [x, w_gate, w_up, w_down]
        dma = pltpu.SemaphoreType.DMA
        flops = 2 * 6 * rows * depth * units
        result = pl.pallas_call(
            kernel,
            out_shape=[pltpu.VMEM(o.shape, BF16) for o in outs],
            in_specs=[pl.BlockSpec(memory_space=pltpu.HBM)] * 7,
            out_specs=[pl.BlockSpec(memory_space=pltpu.VMEM)] * 4,
            scratch_shapes=[
                pltpu.VMEM((SLOTS - 1, BLOCK, depth), F32),
                pltpu.VMEM((SLOTS - 1, big, depth), F32),
                pltpu.VMEM((SLOTS, 2, 6, big, quarter), BF16),
                pltpu.VMEM((SLOTS, 2, 6, big, quarter), BF16),
                pltpu.VMEM((SLOTS, 2, 6, small, quarter), BF16),
                pltpu.VMEM((SLOTS, 2, 6, small, quarter), BF16),
                pltpu.VMEM((rows, units), BF16),
                pltpu.VMEM((rows, units), BF16),
                pltpu.VMEM((units, rows), BF16),
                pltpu.VMEM((2, BLOCK, depth), BF16),
                pltpu.VMEM((2, BLOCK, units), BF16),
                pltpu.VMEM((2, BLOCK, units), BF16),
                pltpu.VMEM((2, rows, COLS), BF16),
                pltpu.VMEM((2, rows, COLS), BF16),
                dma((5,)),
                dma((4,)),
                dma((2,)),
                dma((2,)),
                dma((SLOTS, 2)),
                dma((SLOTS, 2, 2)),
                dma((SLOTS, 2)),
                dma((SLOTS + 1, 3)),
                dma((SLOTS, 2)),
            ],
            compiler_params=pltpu.CompilerParams(
                collective_id=0, has_side_effects=True, vmem_limit_bytes=42 * 2**20
            ),
            cost_estimate=pl.CostEstimate(flops=flops, bytes_accessed=60 * 2**20, transcendentals=rows * units),
        )(x, dy, gate, up, w_gate, w_up, w_down)
        return pl.pallas_call(
            write_out,
            out_shape=[pltpu.HBM(o.shape, BF16) for o in outs],
            in_specs=[pl.BlockSpec(memory_space=pltpu.VMEM)] * 4,
            out_specs=[pl.BlockSpec(memory_space=pltpu.HBM)] * 4,
            scratch_shapes=[dma((16,))],
            compiler_params=pltpu.CompilerParams(has_side_effects=True, vmem_limit_bytes=2**20),
        )(*result)

    tokens, columns, rows = P("dp", None), P(None, "tp"), P("tp", None)
    return jax.shard_map(
        step,
        mesh=mesh,
        in_specs=(tokens, tokens, P("dp", "tp"), P("dp", "tp"), columns, columns, rows),
        out_specs=(tokens, P("dp", "tp"), P("dp", "tp"), P(("dp", "tp"), None)),
        check_vma=False,
    )
```

```python
import jax
import jax.numpy as jnp
from jax import lax
from jax.experimental import pallas as pl
from jax.experimental.pallas import tpu as pltpu
from jax.sharding import PartitionSpec as P

MESH = pl.DeviceIdType.MESH
F32, BF16 = jnp.float32, jnp.bfloat16
BLOCK = 256
COLS = 256
SLOTS = 4
SIDE = 4
CUTS = 1
EARLY = 1
ORDER = [(j, t) for pair in ((0, 2), (1, 3)) for t in range(CUTS) for j in pair]
NT = (((1,), (1,)), ((), ()))
NN = (((1,), (0,)), ((), ()))


def dot(a, b, dims):
    return lax.dot_general(a, b, dims, preferred_element_type=F32)


def kernel(
    x, dy, gate, up, w_gate, w_up, w_down,
    dx, o_gate, o_up, o_down,
    acc, acc2, major_send, major_recv, minor_send, minor_recv,
    d_gate, d_up, hidden_t, dy_in, gate_in, up_in, x_cols, dy_cols,
    first_sem, w_sem, in_sem, cols_sem, rs_send_sem, rs_recv_sem, ag_send_sem, ag_major_sem, ag_minor_sem,
):
    rows, depth = x.shape
    blocks = rows // BLOCK
    big, small = BLOCK // SIDE, BLOCK // SIDE // SIDE
    half, quarter = depth // 2, depth // 4
    pieces = depth // COLS
    units = gate.shape[1]

    me = lax.axis_index("tp")
    px, py = lax.div(me, SIDE), lax.rem(me, SIDE)

    def wrap(k):
        return lax.rem(k + SIDE, SIDE)

    x_ring = [wrap(px + 1) * SIDE + py, wrap(px - 1) * SIDE + py]
    y_ring = [px * SIDE + wrap(py + 1), px * SIDE + wrap(py - 1)]
    major = [(px, x_ring), (py, y_ring)]
    minor = [(py, y_ring), (px, x_ring)]

    def taken(ref, sem):
        pltpu.make_async_copy(ref, ref, sem).wait()

    def taken_rows(n, sem):
        taken(d_gate.at[pl.ds(0, n)], sem)

    quarters = [pl.ds(j * quarter, quarter) for j in range(4)]

    cut = quarter // CUTS

    def cut_at(k):
        j, t = ORDER[k]
        return pl.ds(j * quarter + t * cut, cut)

    def weight_cut(k):
        c = cut_at(k)
        for src, dst in ((w_gate, o_gate), (w_up, o_up)):
            pltpu.make_async_copy(src.at[c], dst.at[c], w_sem.at[k]).start()

    def inputs(b):
        slot = lax.rem(b, 2)
        here = pl.ds(pl.multiple_of(b * BLOCK, BLOCK), BLOCK)
        for src, dst in ((dy, dy_in), (gate, gate_in), (up, up_in)):
            pltpu.make_async_copy(src.at[here], dst.at[slot], in_sem.at[slot]).start()

    def columns(k):
        slot = lax.rem(k, 2)
        here = pl.ds(pl.multiple_of(k * COLS, COLS), COLS)
        for src, dst in ((x, x_cols), (dy, dy_cols)):
            pltpu.make_async_copy(src.at[:, here], dst.at[slot], cols_sem.at[slot]).start()

    for src, dst in ((gate, gate_in), (up, up_in)):
        pltpu.make_async_copy(src.at[pl.ds(0, BLOCK)], dst.at[0], first_sem.at[4]).start()
    for j, c in enumerate(quarters):
        pltpu.make_async_copy(w_down.at[:, c], o_down.at[:, c], first_sem.at[j]).start()
        pltpu.make_async_copy(dy.at[pl.ds(0, BLOCK), c], dy_in.at[0, :, c], first_sem.at[j]).start()
    for k in range(EARLY):
        weight_cut(k)

    barrier = pltpu.get_barrier_semaphore()
    for n in x_ring + y_ring:
        pl.semaphore_signal(barrier, inc=1, device_id={"tp": n}, device_id_type=MESH)

    def remote(src, dst, send, recv, to):
        return pltpu.make_async_remote_copy(
            src_ref=src, dst_ref=dst, send_sem=send, recv_sem=recv, device_id={"tp": to}, device_id_type=MESH
        )

    def rs(b, h, m, phase):
        slot = lax.rem(b, SLOTS)
        sent, got = ((major_send, major_recv), (minor_send, minor_recv))[phase]
        ring = (major, minor)[phase][h][1]
        return remote(
            sent.at[slot, h, m], got.at[slot, h, m],
            rs_send_sem.at[slot, phase], rs_recv_sem.at[slot, phase, int(m >= 2)], ring[m % 2],
        )

    def rs_got(b, phase, late):
        slot = lax.rem(b, SLOTS)
        got = (major_recv, minor_recv)[phase]
        taken(got.at[slot, :, pl.ds(2, 4) if late else pl.ds(0, 2)], rs_recv_sem.at[slot, phase, late])

    def rs_left(b, phase):
        slot = lax.rem(b, SLOTS)
        taken((major_send, minor_send)[phase].at[slot], rs_send_sem.at[slot, phase])

    def ag_left(b, phase):
        slot = lax.rem(b, SLOTS)
        taken((major_send, minor_send)[phase].at[slot], ag_send_sem.at[slot, phase])

    def ag_sem(b, h, m, phase):
        if phase == 0:
            return ag_major_sem.at[lax.rem(b, SLOTS + 1), h if m < 2 else 2]
        return ag_minor_sem.at[lax.rem(b, SLOTS), int(m >= 2)]

    def ag_got(b, phase):
        taken((major_recv, minor_recv)[phase].at[lax.rem(b, SLOTS), :, pl.ds(2, 4)], ag_sem(b, 0, 2, phase))

    def place(b, h, phase, chunk, side):
        start = b * BLOCK + (chunk * big if phase == 0 else major[h][0] * big + chunk * small)
        size = big if phase == 0 else small
        return dx.at[pl.ds(pl.multiple_of(start, size), size), pl.ds(h * half + side * quarter, quarter)]

    def ag(b, h, m, phase):
        slot = lax.rem(b, SLOTS)
        at, ring = (major, minor)[phase][h]
        chunk = [at, at, at, at, wrap(at - 1), wrap(at + 1)][m]
        ref = place(b, h, phase, chunk, (0, 1, 1, 0, 0, 1)[m])
        return remote(ref, ref, ag_send_sem.at[slot, phase], ag_sem(b, h, m, phase), ring[m % 2])

    def source(b, h, phase, chunk, side):
        slot = lax.rem(b, SLOTS - 1)
        ref, size = ((acc, big), (acc2, small))[phase]
        return ref[slot, pl.ds(pl.multiple_of(chunk * size, size), size), pl.ds(h * half + side * quarter, quarter)]

    def scatter_first(b, phase, hs=(0, 1), ms=(0, 1, 2, 3)):
        slot = lax.rem(b, SLOTS)
        sent = (major_send, minor_send)[phase]
        for h in hs:
            at = (major, minor)[phase][h][0]
            chunks = [wrap(at + 2), wrap(at + 2), wrap(at + 1), wrap(at - 1)]
            for m in ms:
                sent[slot, h, m] = source(b, h, phase, chunks[m], (0, 1, 1, 0)[m]).astype(BF16)
        for m in ms:
            for h in hs:
                rs(b, h, m, phase).start()

    def send_cut(b, h, m, t):
        slot = lax.rem(b, SLOTS)
        at, ring = major[h]
        chunk = (wrap(at + 2), wrap(at + 2), wrap(at + 1), wrap(at - 1))[m]
        c = pl.ds(t * cut, cut)
        rows = pl.ds(pl.multiple_of(chunk * big, big), big)
        columns = pl.ds(h * half + (0, 1, 1, 0)[m] * quarter + t * cut, cut)
        major_send[slot, h, m, :, c] = acc[lax.rem(b, SLOTS - 1), rows, columns].astype(BF16)
        remote(
            major_send.at[slot, h, m, :, c], major_recv.at[slot, h, m, :, c],
            rs_send_sem.at[slot, 0], rs_recv_sem.at[slot, 0, int(m >= 2)], ring[m % 2],
        ).start()

    def scatter_second(b, phase):
        slot = lax.rem(b, SLOTS)
        sent, got = ((major_send, major_recv), (minor_send, minor_recv))[phase]
        rs_got(b, phase, 0)
        for h in range(2):
            at = (major, minor)[phase][h][0]
            for m in range(2):
                chunk = wrap(at + 1) if m == 0 else wrap(at - 1)
                sent[slot, h, 4 + m] = (source(b, h, phase, chunk, m) + got[slot, h, m].astype(F32)).astype(BF16)
        for h in range(2):
            for m in range(2):
                rs(b, h, 4 + m, phase).start()

    def total(b, h, phase, side):
        slot = lax.rem(b, SLOTS)
        got = (major_recv, minor_recv)[phase]
        at = (major, minor)[phase][h][0]
        parts = ((3, 4), (2, 5))[side]
        return source(b, h, phase, at, side) + got[slot, h, parts[0]].astype(F32) + got[slot, h, parts[1]].astype(F32)

    def scatter_done(b, phase):
        rs_got(b, phase, 1)
        for h in range(2):
            for side in range(2):
                value = total(b, h, phase, side)
                if phase == 0:
                    acc2[lax.rem(b, SLOTS - 1), :, pl.ds(h * half + side * quarter, quarter)] = value
                else:
                    place(b, h, 1, minor[h][0], side)[...] = value.astype(BF16)

    def gather_first(b, phase):
        for m in range(4):
            for h in range(2):
                ag(b, h, m, phase).start()

    def gather_second(b, phase):
        if phase == 1:
            taken(minor_recv.at[lax.rem(b, SLOTS), :, pl.ds(0, 2)], ag_sem(b, 0, 0, 1))
        for h in range(2):
            if phase == 0:
                taken(major_recv.at[lax.rem(b, SLOTS), 0, pl.ds(0, 2)], ag_sem(b, h, 0, 0))
            for m in range(2):
                ag(b, h, 4 + m, phase).start()

    def activation(slot, rows):
        g, u = gate_in[slot, rows].astype(F32), up_in[slot, rows].astype(F32)
        s = jax.nn.sigmoid(g)
        silu = g * s
        return u, silu, s * (1.0 + g * (1.0 - s)), (silu * u).astype(BF16)

    def hidden_gradient(slot, here, ready):
        u, silu, slope, hidden = activation(slot, pl.ds(0, BLOCK))
        hidden_t[:, here] = hidden.T
        d_hidden = None
        for j, c in enumerate(quarters):
            ready(j)
            piece = dot(dy_in[slot, :, c], o_down[:, c], NT)
            d_hidden = piece if d_hidden is None else d_hidden + piece
        d_gate[here, :] = (d_hidden * u * slope).astype(BF16)
        d_up[here, :] = (d_hidden * silu).astype(BF16)

    def input_gradient(out, here, c):
        acc[out, :, c] = dot(d_gate[here, :], o_gate[c, :], NT) + dot(d_up[here, :], o_up[c, :], NT)

    def first_term():
        here = pl.ds(0, BLOCK)
        taken_rows(2 * BLOCK, first_sem.at[4])

        def ready(j):
            taken_rows((units + BLOCK) * quarter // units, first_sem.at[j])
            if j == 0:
                for k in range(EARLY, 4 * CUTS):
                    weight_cut(k)

        hidden_gradient(0, here, ready)
        inputs(1)
        pl.semaphore_wait(barrier, 4)
        for k, (j, t) in enumerate(ORDER):
            taken_rows(2 * cut, w_sem.at[k])
            input_gradient(0, here, cut_at(k))
            for m in ((0, 3), (1, 2))[j % 2]:
                send_cut(0, j // 2, m, t)

    def term(b):
        slot, out = lax.rem(b, 2), lax.rem(b, SLOTS - 1)
        here = pl.ds(pl.multiple_of(b * BLOCK, BLOCK), BLOCK)
        taken_rows(BLOCK * (depth + 2 * units) // units, in_sem.at[slot])
        hidden_gradient(slot, here, lambda j: None)
        pl.when(b + 1 < blocks)(lambda: inputs(b + 1))
        for j in (0, 2, 1, 3):
            input_gradient(out, here, quarters[j])
            scatter_first(b, 0, (j // 2,), ((0, 3), (1, 2))[j % 2])

    def weight_gradients(k):
        slot = lax.rem(k, 2)
        here = pl.ds(pl.multiple_of(k * COLS, COLS), COLS)
        taken_rows(2 * rows * COLS // units, cols_sem.at[slot])
        pl.when(k + 1 < pieces)(lambda: columns(k + 1))

        x_t = x_cols[slot].T
        o_gate[here, :] = dot(x_t, d_gate[...], NN).astype(BF16)
        o_up[here, :] = dot(x_t, d_up[...], NN).astype(BF16)
        o_down[:, here] = dot(hidden_t[...], dy_cols[slot], NN).astype(BF16)

    per_step = 2
    first_step = blocks

    def at(i, lag, f):
        b = i - lag

        @pl.when(jnp.logical_and(b >= 0, b < blocks))
        def _():
            f(b)

    def weights_at(i, j):
        k = (i - first_step) * per_step + j

        @pl.when(jnp.logical_and(i >= first_step, k < pieces))
        def _():
            weight_gradients(k)

    def step(i, carry):
        at(i, 4, lambda b: rs_left(b, 0))

        pl.when(jnp.logical_and(i > 0, i < blocks))(lambda: term(i))
        pl.when(i == first_step - 1)(lambda: columns(0))

        def turn(b):
            scatter_done(b, 0)
            scatter_first(b, 1)

        at(i, 6, lambda b: rs_left(b, 1))
        at(i, 2, turn)
        at(i, 1, lambda b: scatter_second(b, 0))

        def finish(b):
            scatter_done(b, 1)
            gather_first(b, 1)

        at(i, 8, lambda b: ag_left(b, 1))
        at(i, 4, finish)
        at(i, 3, lambda b: scatter_second(b, 1))
        weights_at(i, 0)
        at(i, 5, lambda b: gather_second(b, 1))
        def gather_rows(b):
            ag_got(b, 1)
            gather_first(b, 0)

        at(i, 6, gather_rows)
        at(i, 7, lambda b: gather_second(b, 0))

        weights_at(i, 1)

        def last(b):
            ag_got(b, 0)
            ag_left(b, 0)

        at(i, 8, last)
        return carry

    first_term()
    lax.fori_loop(0, blocks + 8, step, 0)


def write_out(dx, a, b, c, o_dx, o_a, o_b, o_c, sem):
    pairs = ((dx, o_dx), (a, o_a), (b, o_b), (c, o_c))
    for src, dst in pairs:
        n = src.shape[0] // 8
        for j in range(8):
            cut = pl.ds(j * n, n)
            pltpu.make_async_copy(src.at[cut], dst.at[cut], sem.at[0]).start()
    for src, dst in pairs:
        pltpu.make_async_copy(src, dst, sem.at[0]).wait()


def solution(mesh):
    assert mesh.shape["tp"] == SIDE * SIDE

    def step(x, dy, gate, up, w_gate, w_up, w_down):
        rows, depth = x.shape
        units = gate.shape[1]
        big, small, quarter = BLOCK // SIDE, BLOCK // SIDE // SIDE, depth // 4
        outs = [x, w_gate, w_up, w_down]
        dma = pltpu.SemaphoreType.DMA
        flops = 2 * 6 * rows * depth * units
        result = pl.pallas_call(
            kernel,
            out_shape=[pltpu.VMEM(o.shape, BF16) for o in outs],
            in_specs=[pl.BlockSpec(memory_space=pltpu.HBM)] * 7,
            out_specs=[pl.BlockSpec(memory_space=pltpu.VMEM)] * 4,
            scratch_shapes=[
                pltpu.VMEM((SLOTS - 1, BLOCK, depth), F32),
                pltpu.VMEM((SLOTS - 1, big, depth), F32),
                pltpu.VMEM((SLOTS, 2, 6, big, quarter), BF16),
                pltpu.VMEM((SLOTS, 2, 6, big, quarter), BF16),
                pltpu.VMEM((SLOTS, 2, 6, small, quarter), BF16),
                pltpu.VMEM((SLOTS, 2, 6, small, quarter), BF16),
                pltpu.VMEM((rows, units), BF16),
                pltpu.VMEM((rows, units), BF16),
                pltpu.VMEM((units, rows), BF16),
                pltpu.VMEM((2, BLOCK, depth), BF16),
                pltpu.VMEM((2, BLOCK, units), BF16),
                pltpu.VMEM((2, BLOCK, units), BF16),
                pltpu.VMEM((2, rows, COLS), BF16),
                pltpu.VMEM((2, rows, COLS), BF16),
                dma((5,)),
                dma((4 * CUTS,)),
                dma((2,)),
                dma((2,)),
                dma((SLOTS, 2)),
                dma((SLOTS, 2, 2)),
                dma((SLOTS, 2)),
                dma((SLOTS + 1, 3)),
                dma((SLOTS, 2)),
            ],
            compiler_params=pltpu.CompilerParams(
                collective_id=0, has_side_effects=True, vmem_limit_bytes=42 * 2**20
            ),
            cost_estimate=pl.CostEstimate(flops=flops, bytes_accessed=60 * 2**20, transcendentals=rows * units),
        )(x, dy, gate, up, w_gate, w_up, w_down)
        return pl.pallas_call(
            write_out,
            out_shape=[pltpu.HBM(o.shape, BF16) for o in outs],
            in_specs=[pl.BlockSpec(memory_space=pltpu.VMEM)] * 4,
            out_specs=[pl.BlockSpec(memory_space=pltpu.HBM)] * 4,
            scratch_shapes=[dma((1,))],
            compiler_params=pltpu.CompilerParams(has_side_effects=True, vmem_limit_bytes=2**20),
        )(*result)

    tokens, columns, rows = P("dp", None), P(None, "tp"), P("tp", None)
    return jax.shard_map(
        step,
        mesh=mesh,
        in_specs=(tokens, tokens, P("dp", "tp"), P("dp", "tp"), columns, columns, rows),
        out_specs=(tokens, P("dp", "tp"), P("dp", "tp"), P(("dp", "tp"), None)),
        check_vma=False,
    )
```

```python
import jax
import jax.numpy as jnp
from jax import lax
from jax.experimental import pallas as pl
from jax.experimental.pallas import tpu as pltpu
from jax.sharding import PartitionSpec as P

MESH = pl.DeviceIdType.MESH
F32, BF16 = jnp.float32, jnp.bfloat16
BLOCK = 256
COLS = 256
SLOTS = 4
SIDE = 4
CUTS = 1
EARLY = 1
DEEP = 6
ORDER = [(j, t) for pair in ((0, 2), (1, 3)) for t in range(CUTS) for j in pair]
NT = (((1,), (1,)), ((), ()))
NN = (((1,), (0,)), ((), ()))


def dot(a, b, dims):
    return lax.dot_general(a, b, dims, preferred_element_type=F32)


def kernel(
    x, dy, gate, up, w_gate, w_up, w_down,
    dx, o_gate, o_up, o_down,
    acc, acc2, major_send, major_recv, minor_send, minor_recv,
    d_gate, d_up, hidden_t, dy_in, gate_in, up_in, x_cols, dy_cols,
    first_sem, w_sem, in_sem, cols_sem, rs_send_sem, rs_recv_sem, ag_send_sem, ag_major_sem, ag_minor_sem,
):
    rows, depth = x.shape
    blocks = rows // BLOCK
    big, small = BLOCK // SIDE, BLOCK // SIDE // SIDE
    half, quarter = depth // 2, depth // 4
    pieces = depth // COLS
    units = gate.shape[1]

    me = lax.axis_index("tp")
    px, py = lax.div(me, SIDE), lax.rem(me, SIDE)

    def wrap(k):
        return lax.rem(k + SIDE, SIDE)

    x_ring = [wrap(px + 1) * SIDE + py, wrap(px - 1) * SIDE + py]
    y_ring = [px * SIDE + wrap(py + 1), px * SIDE + wrap(py - 1)]
    major = [(px, x_ring), (py, y_ring)]
    minor = [(py, y_ring), (px, x_ring)]

    def taken(ref, sem):
        pltpu.make_async_copy(ref, ref, sem).wait()

    def taken_rows(n, sem):
        taken(d_gate.at[pl.ds(0, n)], sem)

    quarters = [pl.ds(j * quarter, quarter) for j in range(4)]
    deep = [pl.ds(j * (depth // DEEP), depth // DEEP) for j in range(DEEP)]

    cut = quarter // CUTS

    def cut_at(k):
        j, t = ORDER[k]
        return pl.ds(j * quarter + t * cut, cut)

    def weight_cut(k):
        c = cut_at(k)
        for src, dst in ((w_gate, o_gate), (w_up, o_up)):
            pltpu.make_async_copy(src.at[c], dst.at[c], w_sem.at[k]).start()

    def inputs(b):
        slot = lax.rem(b, 2)
        here = pl.ds(pl.multiple_of(b * BLOCK, BLOCK), BLOCK)
        for src, dst in ((dy, dy_in), (gate, gate_in), (up, up_in)):
            pltpu.make_async_copy(src.at[here], dst.at[slot], in_sem.at[slot]).start()

    def columns(k):
        slot = lax.rem(k, 2)
        here = pl.ds(pl.multiple_of(k * COLS, COLS), COLS)
        for src, dst in ((x, x_cols), (dy, dy_cols)):
            pltpu.make_async_copy(src.at[:, here], dst.at[slot], cols_sem.at[slot]).start()

    for src, dst in ((gate, gate_in), (up, up_in)):
        pltpu.make_async_copy(src.at[pl.ds(0, BLOCK)], dst.at[0], first_sem.at[DEEP]).start()
    for j, c in enumerate(deep):
        pltpu.make_async_copy(w_down.at[:, c], o_down.at[:, c], first_sem.at[j]).start()
        pltpu.make_async_copy(dy.at[pl.ds(0, BLOCK), c], dy_in.at[0, :, c], first_sem.at[j]).start()
    for k in range(EARLY):
        weight_cut(k)

    barrier = pltpu.get_barrier_semaphore()
    for n in x_ring + y_ring:
        pl.semaphore_signal(barrier, inc=1, device_id={"tp": n}, device_id_type=MESH)

    def remote(src, dst, send, recv, to):
        return pltpu.make_async_remote_copy(
            src_ref=src, dst_ref=dst, send_sem=send, recv_sem=recv, device_id={"tp": to}, device_id_type=MESH
        )

    def rs(b, h, m, phase):
        slot = lax.rem(b, SLOTS)
        sent, got = ((major_send, major_recv), (minor_send, minor_recv))[phase]
        ring = (major, minor)[phase][h][1]
        return remote(
            sent.at[slot, h, m], got.at[slot, h, m],
            rs_send_sem.at[slot, phase], rs_recv_sem.at[slot, phase, int(m >= 2)], ring[m % 2],
        )

    def rs_got(b, phase, late):
        slot = lax.rem(b, SLOTS)
        got = (major_recv, minor_recv)[phase]
        taken(got.at[slot, :, pl.ds(2, 4) if late else pl.ds(0, 2)], rs_recv_sem.at[slot, phase, late])

    def rs_left(b, phase):
        slot = lax.rem(b, SLOTS)
        taken((major_send, minor_send)[phase].at[slot], rs_send_sem.at[slot, phase])

    def ag_sent(b, phase):
        return ag_send_sem.at[lax.rem(b, 3) if phase == 0 else 3 + lax.rem(b, 3)]

    def ag_left(b, phase):
        slot = lax.rem(b, SLOTS)
        taken((major_send, minor_send)[phase].at[slot], ag_sent(b, phase))

    def ag_sem(b, h, m, phase):
        if phase == 0:
            return ag_major_sem.at[lax.rem(b, SLOTS + 1), h if m < 2 else 2]
        return ag_minor_sem.at[lax.rem(b, SLOTS), int(m >= 2)]

    def ag_got(b, phase):
        taken((major_recv, minor_recv)[phase].at[lax.rem(b, SLOTS), :, pl.ds(2, 4)], ag_sem(b, 0, 2, phase))

    def place(b, h, phase, chunk, side):
        start = b * BLOCK + (chunk * big if phase == 0 else major[h][0] * big + chunk * small)
        size = big if phase == 0 else small
        return dx.at[pl.ds(pl.multiple_of(start, size), size), pl.ds(h * half + side * quarter, quarter)]

    def ag(b, h, m, phase):
        slot = lax.rem(b, SLOTS)
        at, ring = (major, minor)[phase][h]
        chunk = [at, at, at, at, wrap(at - 1), wrap(at + 1)][m]
        ref = place(b, h, phase, chunk, (0, 1, 1, 0, 0, 1)[m])
        return remote(ref, ref, ag_sent(b, phase), ag_sem(b, h, m, phase), ring[m % 2])

    def source(b, h, phase, chunk, side):
        slot = lax.rem(b, SLOTS - 1)
        ref, size = ((acc, big), (acc2, small))[phase]
        return ref[slot, pl.ds(pl.multiple_of(chunk * size, size), size), pl.ds(h * half + side * quarter, quarter)]

    def scatter_first(b, phase, hs=(0, 1), ms=(0, 1, 2, 3)):
        slot = lax.rem(b, SLOTS)
        sent = (major_send, minor_send)[phase]
        for h in hs:
            at = (major, minor)[phase][h][0]
            chunks = [wrap(at + 2), wrap(at + 2), wrap(at + 1), wrap(at - 1)]
            for m in ms:
                sent[slot, h, m] = source(b, h, phase, chunks[m], (0, 1, 1, 0)[m]).astype(BF16)
        for m in ms:
            for h in hs:
                rs(b, h, m, phase).start()

    def send_cut(b, h, m, t):
        slot = lax.rem(b, SLOTS)
        at, ring = major[h]
        chunk = (wrap(at + 2), wrap(at + 2), wrap(at + 1), wrap(at - 1))[m]
        c = pl.ds(t * cut, cut)
        rows = pl.ds(pl.multiple_of(chunk * big, big), big)
        columns = pl.ds(h * half + (0, 1, 1, 0)[m] * quarter + t * cut, cut)
        major_send[slot, h, m, :, c] = acc[lax.rem(b, SLOTS - 1), rows, columns].astype(BF16)
        remote(
            major_send.at[slot, h, m, :, c], major_recv.at[slot, h, m, :, c],
            rs_send_sem.at[slot, 0], rs_recv_sem.at[slot, 0, int(m >= 2)], ring[m % 2],
        ).start()

    def scatter_second(b, phase):
        slot = lax.rem(b, SLOTS)
        sent, got = ((major_send, major_recv), (minor_send, minor_recv))[phase]
        rs_got(b, phase, 0)
        for h in range(2):
            at = (major, minor)[phase][h][0]
            for m in range(2):
                chunk = wrap(at + 1) if m == 0 else wrap(at - 1)
                sent[slot, h, 4 + m] = (source(b, h, phase, chunk, m) + got[slot, h, m].astype(F32)).astype(BF16)
        for h in range(2):
            for m in range(2):
                rs(b, h, 4 + m, phase).start()

    def total(b, h, phase, side):
        slot = lax.rem(b, SLOTS)
        got = (major_recv, minor_recv)[phase]
        at = (major, minor)[phase][h][0]
        parts = ((3, 4), (2, 5))[side]
        return source(b, h, phase, at, side) + got[slot, h, parts[0]].astype(F32) + got[slot, h, parts[1]].astype(F32)

    def scatter_done(b, phase):
        rs_got(b, phase, 1)
        for h in range(2):
            for side in range(2):
                value = total(b, h, phase, side)
                if phase == 0:
                    acc2[lax.rem(b, SLOTS - 1), :, pl.ds(h * half + side * quarter, quarter)] = value
                else:
                    place(b, h, 1, minor[h][0], side)[...] = value.astype(BF16)

    def gather_first(b, phase):
        for m in range(4):
            for h in range(2):
                ag(b, h, m, phase).start()

    def gather_second(b, phase):
        if phase == 1:
            taken(minor_recv.at[lax.rem(b, SLOTS), :, pl.ds(0, 2)], ag_sem(b, 0, 0, 1))
        for h in range(2):
            if phase == 0:
                taken(major_recv.at[lax.rem(b, SLOTS), 0, pl.ds(0, 2)], ag_sem(b, h, 0, 0))
            for m in range(2):
                ag(b, h, 4 + m, phase).start()

    def activation(slot, rows):
        g, u = gate_in[slot, rows].astype(F32), up_in[slot, rows].astype(F32)
        s = jax.nn.sigmoid(g)
        silu = g * s
        return u, silu, s * (1.0 + g * (1.0 - s)), (silu * u).astype(BF16)

    def hidden_gradient(slot, here, ready):
        u, silu, slope, hidden = activation(slot, pl.ds(0, BLOCK))
        hidden_t[:, here] = hidden.T
        d_hidden = None
        if ready is None:
            d_hidden = dot(dy_in[slot], o_down[...], NT)
        for j, c in enumerate(deep if ready else ()):
            ready(j)
            piece = dot(dy_in[slot, :, c], o_down[:, c], NT)
            d_hidden = piece if d_hidden is None else d_hidden + piece
        d_gate[here, :] = (d_hidden * u * slope).astype(BF16)
        d_up[here, :] = (d_hidden * silu).astype(BF16)

    def input_gradient(out, here, c):
        acc[out, :, c] = dot(d_gate[here, :], o_gate[c, :], NT) + dot(d_up[here, :], o_up[c, :], NT)

    def first_term():
        here = pl.ds(0, BLOCK)
        taken_rows(2 * BLOCK, first_sem.at[DEEP])

        def ready(j):
            taken_rows((units + BLOCK) * (depth // DEEP) // units, first_sem.at[j])
            if j == 0:
                for k in range(EARLY, 4 * CUTS):
                    weight_cut(k)

        hidden_gradient(0, here, ready)
        inputs(1)
        pl.semaphore_wait(barrier, 4)
        for k, (j, t) in enumerate(ORDER):
            taken_rows(2 * cut, w_sem.at[k])
            input_gradient(0, here, cut_at(k))
            for m in ((0, 3), (1, 2))[j % 2]:
                send_cut(0, j // 2, m, t)

    def term(b):
        slot, out = lax.rem(b, 2), lax.rem(b, SLOTS - 1)
        here = pl.ds(pl.multiple_of(b * BLOCK, BLOCK), BLOCK)
        taken_rows(BLOCK * (depth + 2 * units) // units, in_sem.at[slot])
        hidden_gradient(slot, here, None)
        pl.when(b + 1 < blocks)(lambda: inputs(b + 1))
        for j in (0, 2, 1, 3):
            input_gradient(out, here, quarters[j])
            scatter_first(b, 0, (j // 2,), ((0, 3), (1, 2))[j % 2])

    def weight_gradients(k):
        slot = lax.rem(k, 2)
        here = pl.ds(pl.multiple_of(k * COLS, COLS), COLS)
        taken_rows(2 * rows * COLS // units, cols_sem.at[slot])
        pl.when(k + 1 < pieces)(lambda: columns(k + 1))

        x_t = x_cols[slot].T
        o_gate[here, :] = dot(x_t, d_gate[...], NN).astype(BF16)
        o_up[here, :] = dot(x_t, d_up[...], NN).astype(BF16)
        o_down[:, here] = dot(hidden_t[...], dy_cols[slot], NN).astype(BF16)

    per_step = 2
    first_step = blocks

    def at(i, lag, f):
        b = i - lag

        @pl.when(jnp.logical_and(b >= 0, b < blocks))
        def _():
            f(b)

    def weights_at(i, j):
        k = (i - first_step) * per_step + j

        @pl.when(jnp.logical_and(i >= first_step, k < pieces))
        def _():
            weight_gradients(k)

    def step(i, carry):
        at(i, 4, lambda b: rs_left(b, 0))

        pl.when(jnp.logical_and(i > 0, i < blocks))(lambda: term(i))
        pl.when(i == first_step - 1)(lambda: columns(0))

        def turn(b):
            scatter_done(b, 0)
            scatter_first(b, 1)

        at(i, 6, lambda b: rs_left(b, 1))
        at(i, 2, turn)
        at(i, 1, lambda b: scatter_second(b, 0))

        def finish(b):
            scatter_done(b, 1)
            gather_first(b, 1)

        at(i, 7, lambda b: ag_left(b, 1))
        at(i, 4, finish)
        at(i, 3, lambda b: scatter_second(b, 1))
        weights_at(i, 0)
        at(i, 5, lambda b: gather_second(b, 1))
        def gather_rows(b):
            ag_got(b, 1)
            gather_first(b, 0)

        at(i, 6, gather_rows)
        at(i, 7, lambda b: gather_second(b, 0))

        weights_at(i, 1)

        def last(b):
            ag_got(b, 0)
            ag_left(b, 0)

        at(i, 8, last)
        return carry

    first_term()
    lax.fori_loop(0, blocks + 8, step, 0)


def write_out(dx, a, b, c, o_dx, o_a, o_b, o_c, sem):
    pairs = ((dx, o_dx), (a, o_a), (b, o_b), (c, o_c))
    for src, dst in pairs:
        n = src.shape[0] // 16
        for j in range(16):
            cut = pl.ds(j * n, n)
            pltpu.make_async_copy(src.at[cut], dst.at[cut], sem.at[0]).start()
    for src, dst in pairs:
        pltpu.make_async_copy(src, dst, sem.at[0]).wait()


def solution(mesh):
    assert mesh.shape["tp"] == SIDE * SIDE

    def step(x, dy, gate, up, w_gate, w_up, w_down):
        rows, depth = x.shape
        units = gate.shape[1]
        big, small, quarter = BLOCK // SIDE, BLOCK // SIDE // SIDE, depth // 4
        outs = [x, w_gate, w_up, w_down]
        dma = pltpu.SemaphoreType.DMA
        flops = 2 * 6 * rows * depth * units
        result = pl.pallas_call(
            kernel,
            out_shape=[pltpu.VMEM(o.shape, BF16) for o in outs],
            in_specs=[pl.BlockSpec(memory_space=pltpu.HBM)] * 7,
            out_specs=[pl.BlockSpec(memory_space=pltpu.VMEM)] * 4,
            scratch_shapes=[
                pltpu.VMEM((SLOTS - 1, BLOCK, depth), F32),
                pltpu.VMEM((SLOTS - 1, big, depth), F32),
                pltpu.VMEM((SLOTS, 2, 6, big, quarter), BF16),
                pltpu.VMEM((SLOTS, 2, 6, big, quarter), BF16),
                pltpu.VMEM((SLOTS, 2, 6, small, quarter), BF16),
                pltpu.VMEM((SLOTS, 2, 6, small, quarter), BF16),
                pltpu.VMEM((rows, units), BF16),
                pltpu.VMEM((rows, units), BF16),
                pltpu.VMEM((units, rows), BF16),
                pltpu.VMEM((2, BLOCK, depth), BF16),
                pltpu.VMEM((2, BLOCK, units), BF16),
                pltpu.VMEM((2, BLOCK, units), BF16),
                pltpu.VMEM((2, rows, COLS), BF16),
                pltpu.VMEM((2, rows, COLS), BF16),
                dma((DEEP + 1,)),
                dma((4 * CUTS,)),
                dma((2,)),
                dma((2,)),
                dma((SLOTS, 2)),
                dma((SLOTS, 2, 2)),
                dma((6,)),
                dma((SLOTS + 1, 3)),
                dma((SLOTS, 2)),
            ],
            compiler_params=pltpu.CompilerParams(
                collective_id=0, has_side_effects=True, vmem_limit_bytes=42 * 2**20
            ),
            cost_estimate=pl.CostEstimate(flops=flops, bytes_accessed=60 * 2**20, transcendentals=rows * units),
        )(x, dy, gate, up, w_gate, w_up, w_down)
        return pl.pallas_call(
            write_out,
            out_shape=[pltpu.HBM(o.shape, BF16) for o in outs],
            in_specs=[pl.BlockSpec(memory_space=pltpu.VMEM)] * 4,
            out_specs=[pl.BlockSpec(memory_space=pltpu.HBM)] * 4,
            scratch_shapes=[dma((1,))],
            compiler_params=pltpu.CompilerParams(has_side_effects=True, vmem_limit_bytes=2**20),
        )(*result)

    tokens, columns, rows = P("dp", None), P(None, "tp"), P("tp", None)
    return jax.shard_map(
        step,
        mesh=mesh,
        in_specs=(tokens, tokens, P("dp", "tp"), P("dp", "tp"), columns, columns, rows),
        out_specs=(tokens, P("dp", "tp"), P("dp", "tp"), P(("dp", "tp"), None)),
        check_vma=False,
    )
```

```python
import jax
import jax.numpy as jnp
from jax import lax
from jax.experimental import pallas as pl
from jax.experimental.pallas import tpu as pltpu
from jax.sharding import PartitionSpec as P

MESH = pl.DeviceIdType.MESH
F32, BF16 = jnp.float32, jnp.bfloat16
BLOCK = 256
COLS = 256
SLOTS = 4
SIDE = 4
CUTS = 1
EARLY = 1
DEEP = 6
ORDER = [(j, t) for pair in ((0, 2), (1, 3)) for t in range(CUTS) for j in pair]
NT = (((1,), (1,)), ((), ()))
NN = (((1,), (0,)), ((), ()))


def dot(a, b, dims):
    return lax.dot_general(a, b, dims, preferred_element_type=F32)


def kernel(
    x, dy, gate, up, w_gate, w_up, w_down,
    dx, o_gate, o_up, o_down,
    acc, acc2, major_send, major_recv, minor_send, minor_recv,
    d_gate, d_up, hidden_t, dy_in, gate_in, up_in, x_cols, dy_cols,
    first_sem, w_sem, in_sem, cols_sem, rs_send_sem, rs_recv_sem, ag_send_sem, ag_major_sem, ag_minor_sem,
):
    rows, depth = x.shape
    blocks = rows // BLOCK
    big, small = BLOCK // SIDE, BLOCK // SIDE // SIDE
    half, quarter = depth // 2, depth // 4
    pieces = depth // COLS
    units = gate.shape[1]

    me = lax.axis_index("tp")
    px, py = lax.div(me, SIDE), lax.rem(me, SIDE)

    def wrap(k):
        return lax.rem(k + SIDE, SIDE)

    x_ring = [wrap(px + 1) * SIDE + py, wrap(px - 1) * SIDE + py]
    y_ring = [px * SIDE + wrap(py + 1), px * SIDE + wrap(py - 1)]
    major = [(px, x_ring), (py, y_ring)]
    minor = [(py, y_ring), (px, x_ring)]

    def taken(ref, sem):
        pltpu.make_async_copy(ref, ref, sem).wait()

    def taken_rows(n, sem):
        taken(d_gate.at[pl.ds(0, n)], sem)

    quarters = [pl.ds(j * quarter, quarter) for j in range(4)]
    deep = [pl.ds(j * (depth // DEEP), depth // DEEP) for j in range(DEEP)]

    cut = quarter // CUTS

    def cut_at(k):
        j, t = ORDER[k]
        return pl.ds(j * quarter + t * cut, cut)

    def weight_cut(k):
        c = cut_at(k)
        for src, dst in ((w_gate, o_gate), (w_up, o_up)):
            pltpu.make_async_copy(src.at[c], dst.at[c], w_sem.at[k]).start()

    def inputs(b):
        slot = lax.rem(b, 2)
        here = pl.ds(pl.multiple_of(b * BLOCK, BLOCK), BLOCK)
        for src, dst in ((dy, dy_in), (gate, gate_in), (up, up_in)):
            pltpu.make_async_copy(src.at[here], dst.at[slot], in_sem.at[slot]).start()

    def columns(k):
        slot = lax.rem(k, 2)
        here = pl.ds(pl.multiple_of(k * COLS, COLS), COLS)
        for src, dst in ((x, x_cols), (dy, dy_cols)):
            pltpu.make_async_copy(src.at[:, here], dst.at[slot], cols_sem.at[slot]).start()

    for src, dst in ((gate, gate_in), (up, up_in)):
        pltpu.make_async_copy(src.at[pl.ds(0, BLOCK)], dst.at[0], first_sem.at[DEEP]).start()
    for j, c in enumerate(deep):
        pltpu.make_async_copy(w_down.at[:, c], o_down.at[:, c], first_sem.at[j]).start()
        pltpu.make_async_copy(dy.at[pl.ds(0, BLOCK), c], dy_in.at[0, :, c], first_sem.at[j]).start()
    for k in range(EARLY):
        weight_cut(k)

    barrier = pltpu.get_barrier_semaphore()
    for n in x_ring + y_ring:
        pl.semaphore_signal(barrier, inc=1, device_id={"tp": n}, device_id_type=MESH)

    def remote(src, dst, send, recv, to):
        return pltpu.make_async_remote_copy(
            src_ref=src, dst_ref=dst, send_sem=send, recv_sem=recv, device_id={"tp": to}, device_id_type=MESH
        )

    def rs(b, h, m, phase):
        slot = lax.rem(b, SLOTS)
        sent, got = ((major_send, major_recv), (minor_send, minor_recv))[phase]
        ring = (major, minor)[phase][h][1]
        return remote(
            sent.at[slot, h, m], got.at[slot, h, m],
            rs_send_sem.at[slot, phase], rs_recv_sem.at[slot, phase, int(m >= 2)], ring[m % 2],
        )

    def rs_got(b, phase, late):
        slot = lax.rem(b, SLOTS)
        got = (major_recv, minor_recv)[phase]
        taken(got.at[slot, :, pl.ds(2, 4) if late else pl.ds(0, 2)], rs_recv_sem.at[slot, phase, late])

    def rs_left(b, phase):
        slot = lax.rem(b, SLOTS)
        taken((major_send, minor_send)[phase].at[slot], rs_send_sem.at[slot, phase])

    def ag_sent(b, phase):
        return ag_send_sem.at[lax.rem(b, 3) if phase == 0 else 3 + lax.rem(b, 3)]

    def ag_left(b, phase):
        slot = lax.rem(b, SLOTS)
        taken((major_send, minor_send)[phase].at[slot], ag_sent(b, phase))

    def ag_sem(b, h, m, phase):
        if phase == 0:
            return ag_major_sem.at[lax.rem(b, SLOTS + 1), h if m < 2 else 2]
        return ag_minor_sem.at[lax.rem(b, SLOTS), int(m >= 2)]

    def ag_got(b, phase):
        taken((major_recv, minor_recv)[phase].at[lax.rem(b, SLOTS), :, pl.ds(2, 4)], ag_sem(b, 0, 2, phase))

    def place(b, h, phase, chunk, side):
        start = b * BLOCK + (chunk * big if phase == 0 else major[h][0] * big + chunk * small)
        size = big if phase == 0 else small
        return dx.at[pl.ds(pl.multiple_of(start, size), size), pl.ds(h * half + side * quarter, quarter)]

    def ag(b, h, m, phase):
        slot = lax.rem(b, SLOTS)
        at, ring = (major, minor)[phase][h]
        chunk = [at, at, at, at, wrap(at - 1), wrap(at + 1)][m]
        ref = place(b, h, phase, chunk, (0, 1, 1, 0, 0, 1)[m])
        return remote(ref, ref, ag_sent(b, phase), ag_sem(b, h, m, phase), ring[m % 2])

    def source(b, h, phase, chunk, side):
        slot = lax.rem(b, SLOTS - 1)
        ref, size = ((acc, big), (acc2, small))[phase]
        return ref[slot, pl.ds(pl.multiple_of(chunk * size, size), size), pl.ds(h * half + side * quarter, quarter)]

    def scatter_first(b, phase, hs=(0, 1), ms=(0, 1, 2, 3)):
        slot = lax.rem(b, SLOTS)
        sent = (major_send, minor_send)[phase]
        for h in hs:
            at = (major, minor)[phase][h][0]
            chunks = [wrap(at + 2), wrap(at + 2), wrap(at + 1), wrap(at - 1)]
            for m in ms:
                sent[slot, h, m] = source(b, h, phase, chunks[m], (0, 1, 1, 0)[m]).astype(BF16)
        for m in ms:
            for h in hs:
                rs(b, h, m, phase).start()

    def send_cut(b, h, m, t):
        slot = lax.rem(b, SLOTS)
        at, ring = major[h]
        chunk = (wrap(at + 2), wrap(at + 2), wrap(at + 1), wrap(at - 1))[m]
        c = pl.ds(t * cut, cut)
        rows = pl.ds(pl.multiple_of(chunk * big, big), big)
        columns = pl.ds(h * half + (0, 1, 1, 0)[m] * quarter + t * cut, cut)
        major_send[slot, h, m, :, c] = acc[lax.rem(b, SLOTS - 1), rows, columns].astype(BF16)
        remote(
            major_send.at[slot, h, m, :, c], major_recv.at[slot, h, m, :, c],
            rs_send_sem.at[slot, 0], rs_recv_sem.at[slot, 0, int(m >= 2)], ring[m % 2],
        ).start()

    def scatter_second(b, phase):
        slot = lax.rem(b, SLOTS)
        sent, got = ((major_send, major_recv), (minor_send, minor_recv))[phase]
        rs_got(b, phase, 0)
        for h in range(2):
            at = (major, minor)[phase][h][0]
            for m in range(2):
                chunk = wrap(at + 1) if m == 0 else wrap(at - 1)
                sent[slot, h, 4 + m] = (source(b, h, phase, chunk, m) + got[slot, h, m].astype(F32)).astype(BF16)
        for h in range(2):
            for m in range(2):
                rs(b, h, 4 + m, phase).start()

    def total(b, h, phase, side):
        slot = lax.rem(b, SLOTS)
        got = (major_recv, minor_recv)[phase]
        at = (major, minor)[phase][h][0]
        parts = ((3, 4), (2, 5))[side]
        return source(b, h, phase, at, side) + got[slot, h, parts[0]].astype(F32) + got[slot, h, parts[1]].astype(F32)

    def scatter_done(b, phase):
        rs_got(b, phase, 1)
        for h in range(2):
            for side in range(2):
                value = total(b, h, phase, side)
                if phase == 0:
                    acc2[lax.rem(b, SLOTS - 1), :, pl.ds(h * half + side * quarter, quarter)] = value
                else:
                    place(b, h, 1, minor[h][0], side)[...] = value.astype(BF16)

    def gather_first(b, phase):
        for m in range(4):
            for h in range(2):
                ag(b, h, m, phase).start()

    def gather_second(b, phase):
        if phase == 1:
            taken(minor_recv.at[lax.rem(b, SLOTS), :, pl.ds(0, 2)], ag_sem(b, 0, 0, 1))
        for h in range(2):
            if phase == 0:
                taken(major_recv.at[lax.rem(b, SLOTS), 0, pl.ds(0, 2)], ag_sem(b, h, 0, 0))
            for m in range(2):
                ag(b, h, 4 + m, phase).start()

    def activation(slot, rows):
        g, u = gate_in[slot, rows].astype(F32), up_in[slot, rows].astype(F32)
        s = jax.nn.sigmoid(g)
        silu = g * s
        return u, silu, s * (1.0 + g * (1.0 - s)), (silu * u).astype(BF16)

    def hidden_gradient(slot, here, ready):
        u, silu, slope, hidden = activation(slot, pl.ds(0, BLOCK))
        hidden_t[:, here] = hidden.T
        d_hidden = None
        if ready is None:
            d_hidden = dot(dy_in[slot], o_down[...], NT)
        for j, c in enumerate(deep if ready else ()):
            ready(j)
            piece = dot(dy_in[slot, :, c], o_down[:, c], NT)
            d_hidden = piece if d_hidden is None else d_hidden + piece
        d_gate[here, :] = (d_hidden * u * slope).astype(BF16)
        d_up[here, :] = (d_hidden * silu).astype(BF16)

    def input_gradient(out, here, c):
        acc[out, :, c] = dot(d_gate[here, :], o_gate[c, :], NT) + dot(d_up[here, :], o_up[c, :], NT)

    def first_term():
        here = pl.ds(0, BLOCK)
        taken_rows(2 * BLOCK, first_sem.at[DEEP])

        def ready(j):
            taken_rows((units + BLOCK) * (depth // DEEP) // units, first_sem.at[j])
            if j == 0:
                for k in range(EARLY, 4 * CUTS):
                    weight_cut(k)

        hidden_gradient(0, here, ready)
        pl.semaphore_wait(barrier, 4)
        for k, (j, t) in enumerate(ORDER):
            taken_rows(2 * cut, w_sem.at[k])
            input_gradient(0, here, cut_at(k))
            for m in ((0, 3), (1, 2))[j % 2]:
                send_cut(0, j // 2, m, t)
            if k == 1:
                inputs(1)

    def term(b):
        slot, out = lax.rem(b, 2), lax.rem(b, SLOTS - 1)
        here = pl.ds(pl.multiple_of(b * BLOCK, BLOCK), BLOCK)
        taken_rows(BLOCK * (depth + 2 * units) // units, in_sem.at[slot])
        hidden_gradient(slot, here, None)
        pl.when(b + 1 < blocks)(lambda: inputs(b + 1))
        for j in (0, 2, 1, 3):
            input_gradient(out, here, quarters[j])
            scatter_first(b, 0, (j // 2,), ((0, 3), (1, 2))[j % 2])

    def weight_gradients(k):
        slot = lax.rem(k, 2)
        here = pl.ds(pl.multiple_of(k * COLS, COLS), COLS)
        taken_rows(2 * rows * COLS // units, cols_sem.at[slot])
        pl.when(k + 1 < pieces)(lambda: columns(k + 1))

        x_t = x_cols[slot].T
        o_gate[here, :] = dot(x_t, d_gate[...], NN).astype(BF16)
        o_up[here, :] = dot(x_t, d_up[...], NN).astype(BF16)
        o_down[:, here] = dot(hidden_t[...], dy_cols[slot], NN).astype(BF16)

    per_step = 2
    first_step = blocks

    def at(i, lag, f):
        b = i - lag

        @pl.when(jnp.logical_and(b >= 0, b < blocks))
        def _():
            f(b)

    def weights_at(i, j):
        k = (i - first_step) * per_step + j

        @pl.when(jnp.logical_and(i >= first_step, k < pieces))
        def _():
            weight_gradients(k)

    def step(i, carry):
        at(i, 4, lambda b: rs_left(b, 0))

        pl.when(jnp.logical_and(i > 0, i < blocks))(lambda: term(i))
        pl.when(i == first_step - 1)(lambda: columns(0))

        def turn(b):
            scatter_done(b, 0)
            scatter_first(b, 1)

        at(i, 6, lambda b: rs_left(b, 1))
        at(i, 2, turn)
        at(i, 1, lambda b: scatter_second(b, 0))

        def finish(b):
            scatter_done(b, 1)
            gather_first(b, 1)

        at(i, 7, lambda b: ag_left(b, 1))
        at(i, 4, finish)
        at(i, 3, lambda b: scatter_second(b, 1))
        weights_at(i, 0)
        at(i, 5, lambda b: gather_second(b, 1))
        def gather_rows(b):
            ag_got(b, 1)
            gather_first(b, 0)

        at(i, 6, gather_rows)
        at(i, 7, lambda b: gather_second(b, 0))

        weights_at(i, 1)

        def last(b):
            ag_got(b, 0)
            ag_left(b, 0)

        at(i, 8, last)
        return carry

    first_term()
    lax.fori_loop(0, blocks + 8, step, 0)


def write_out(dx, a, b, c, o_dx, o_a, o_b, o_c, sem):
    pairs = ((dx, o_dx), (a, o_a), (b, o_b), (c, o_c))
    for src, dst in pairs:
        n = src.shape[0] // 16
        for j in range(16):
            cut = pl.ds(j * n, n)
            pltpu.make_async_copy(src.at[cut], dst.at[cut], sem.at[0]).start()
    for src, dst in pairs:
        pltpu.make_async_copy(src, dst, sem.at[0]).wait()


def solution(mesh):
    assert mesh.shape["tp"] == SIDE * SIDE

    def step(x, dy, gate, up, w_gate, w_up, w_down):
        rows, depth = x.shape
        units = gate.shape[1]
        big, small, quarter = BLOCK // SIDE, BLOCK // SIDE // SIDE, depth // 4
        outs = [x, w_gate, w_up, w_down]
        dma = pltpu.SemaphoreType.DMA
        flops = 2 * 6 * rows * depth * units
        result = pl.pallas_call(
            kernel,
            out_shape=[pltpu.VMEM(o.shape, BF16) for o in outs],
            in_specs=[pl.BlockSpec(memory_space=pltpu.HBM)] * 7,
            out_specs=[pl.BlockSpec(memory_space=pltpu.VMEM)] * 4,
            scratch_shapes=[
                pltpu.VMEM((SLOTS - 1, BLOCK, depth), F32),
                pltpu.VMEM((SLOTS - 1, big, depth), F32),
                pltpu.VMEM((SLOTS, 2, 6, big, quarter), BF16),
                pltpu.VMEM((SLOTS, 2, 6, big, quarter), BF16),
                pltpu.VMEM((SLOTS, 2, 6, small, quarter), BF16),
                pltpu.VMEM((SLOTS, 2, 6, small, quarter), BF16),
                pltpu.VMEM((rows, units), BF16),
                pltpu.VMEM((rows, units), BF16),
                pltpu.VMEM((units, rows), BF16),
                pltpu.VMEM((2, BLOCK, depth), BF16),
                pltpu.VMEM((2, BLOCK, units), BF16),
                pltpu.VMEM((2, BLOCK, units), BF16),
                pltpu.VMEM((2, rows, COLS), BF16),
                pltpu.VMEM((2, rows, COLS), BF16),
                dma((DEEP + 1,)),
                dma((4 * CUTS,)),
                dma((2,)),
                dma((2,)),
                dma((SLOTS, 2)),
                dma((SLOTS, 2, 2)),
                dma((6,)),
                dma((SLOTS + 1, 3)),
                dma((SLOTS, 2)),
            ],
            compiler_params=pltpu.CompilerParams(
                collective_id=0, has_side_effects=True, vmem_limit_bytes=42 * 2**20
            ),
            cost_estimate=pl.CostEstimate(flops=flops, bytes_accessed=60 * 2**20, transcendentals=rows * units),
        )(x, dy, gate, up, w_gate, w_up, w_down)
        return pl.pallas_call(
            write_out,
            out_shape=[pltpu.HBM(o.shape, BF16) for o in outs],
            in_specs=[pl.BlockSpec(memory_space=pltpu.VMEM)] * 4,
            out_specs=[pl.BlockSpec(memory_space=pltpu.HBM)] * 4,
            scratch_shapes=[dma((1,))],
            compiler_params=pltpu.CompilerParams(has_side_effects=True, vmem_limit_bytes=2**20),
        )(*result)

    tokens, columns, rows = P("dp", None), P(None, "tp"), P("tp", None)
    return jax.shard_map(
        step,
        mesh=mesh,
        in_specs=(tokens, tokens, P("dp", "tp"), P("dp", "tp"), columns, columns, rows),
        out_specs=(tokens, P("dp", "tp"), P("dp", "tp"), P(("dp", "tp"), None)),
        check_vma=False,
    )
```
